32 devices in a mesh: gx: 16 (over z, x, core), gy: 2 (over y).
Axes of the slice: x: 2, y: 2, z: 4, core: 2. Of those that a mesh axis runs over, the one named last changes fastest.
Arguments:
- velocity: float32 [256, 256, 512], P('gx', 'gy'), may hold values from -24 to 24
- viscosity: float32 [256], P('gx'), may hold values from 1000 to 8000
- marker_forces: bfloat16 [4096, 16], P(('gx', 'gy')), may hold values from -18 to 18
- spread_weights: bfloat16 [4096, 16, 2048], P(('gx', 'gy')), may hold values from -1.5 to 1.5
- block_owner: int32 [4096, 1], P(('gx', 'gy')), may hold values from 0 to 31; in each aligned block of 128 rows (0 to 127, 128 to 255, ...) at most 8 rows name the same one
- tile_slot: int32 [4096], P(('gx', 'gy')), may hold values from 0 to 511
Outputs:
- relaxed: float32 [256, 256, 512], P('gx', 'gy')
The draws below stay inside these ranges and needn't reach their ends.
Inputs may be any that keep to these rules, and one draw needn't show every extreme that they name: `block_owner`: among the 128 blocks held by one device, no owner is named by more than 8 of them.
All inputs are finite; a program needn't handle non-finite values.
Results may differ from the reference program's by a relative error of at most 0.0013.
Values may be sent and summed in bfloat16 or wider, within the bound.
A program may use at most 128 MiB of HBM per device.

```python
import math
import jax
import jax.numpy as jnp
import numpy as np
from jax import lax

CX = 16
CY = 128
CZ = 512
SEG = 128
MB = 16
BLK_DEV = 128
CAP = 8
TILE = 2048
NX = 256
NY = 256
NZ = 512
NBLK = 4096
N_GX = 16
N_GY = 2
DEVICES = 32


def plant(result, own_key, smallest, top_value):
    longest = result.shape.index(max(result.shape))
    spots = []
    for shift in (0, 1):
        where = [jax.random.randint(jax.random.fold_in(own_key, axis), (), 0, length) for axis, length in enumerate(result.shape)]
        where[longest] = (where[longest] + shift) % result.shape[longest]
        spots.append(tuple(where))
    return result.at[spots[0]].set(smallest).at[spots[1]].set(top_value)


def levels(stream_key, dims, pieces, least, largest):
    gain, own = 1.0, jax.random.fold_in(stream_key, 6)
    for dim, blocks in pieces:
        heights = jnp.exp(jax.random.uniform(jax.random.fold_in(own, dim), (blocks,), jnp.float32, least / len(pieces), largest / len(pieces)))
        gain = gain * jnp.repeat(heights, dims[dim] // blocks).reshape([-1 if axis == dim else 1 for axis in range(len(dims))])
    return gain


def assign_block(rng, own, number, rows, count, top, bound, lean):
    order = jax.random.permutation(rng, count)
    crowded, usual = portions_of(count, rows * top, bound, lean, True), portions_of(count, rows * top, bound, lean, False)
    places = jnp.arange(count)

    def named(tallies, turn):
        used = int((tallies > 0).sum())
        fixed = max(1, used // 4)
        shifted = fixed + (places - fixed + turn * (used - fixed)) % max(1, count - fixed)
        return jnp.zeros((count,), jnp.int32).at[order[jnp.where(places < fixed, places, shifted)]].set(jnp.asarray(tallies, jnp.int32))

    tallies = jnp.where(number % 4 == 0, named(crowded, number // 4), named(usual, number - number // 4 - 1))
    mixed = jax.random.permutation(jax.random.fold_in(own, 3), count)
    donor, sink = mixed[0:count // 2 * 2:2], mixed[1:count // 2 * 2:2]
    margin = jnp.minimum(tallies[donor] - 1, bound - tallies[sink]) // 2
    margin = jnp.where((donor == order[0]) | (sink == order[0]) | (tallies[sink] == 0), 0, jnp.maximum(margin, 0))
    shifted = jax.random.randint(jax.random.fold_in(own, 4), (count // 2,), 0, 1 << 20) % (margin + 1)
    tallies = tallies.at[donor].add(-shifted).at[sink].add(shifted)
    members = jnp.searchsorted(jnp.cumsum(tallies), jnp.arange(rows * top), side="right").astype(jnp.int32)
    grid = members.reshape(top, rows).T
    grid = grid[jax.random.permutation(jax.random.fold_in(own, 1), rows)]
    turn = jax.random.randint(jax.random.fold_in(own, 2), (rows, 1), 0, top)
    return jnp.take_along_axis(grid, (jnp.arange(top)[None, :] + turn) % top, axis=1)


def portions_of(amount, total, bound, slope, full):
    weights = [(1 << 20) // math.isqrt(rank ** slope) + 1 for rank in range(1, amount + 1)]
    largest = bound if full else min(bound, max(-(-total // amount), total * weights[0] // sum(weights)))
    least = 1 if total - largest >= amount - 1 else 0
    counts, surplus = [largest] + [least] * (amount - 1), total - largest - least * (amount - 1)
    while surplus > 0:
        free = [i for i in range(1, amount) if counts[i] < largest] or [i for i in range(1, amount) if counts[i] < bound]
        mass, remaining = sum([weights[i] for i in free]), surplus
        for i in free:
            more = min(bound - counts[i], max(1, remaining * weights[i] // mass), surplus)
            counts[i] = counts[i] + more
            surplus = surplus - more
    return np.array(counts)


def normal_values(own_key, extent, deviation, most, split=(), held_as=jnp.bfloat16):
    array = deviation * jax.random.normal(own_key, extent, jnp.float32)
    if split:
        array = array * levels(own_key, extent, split, -0.22, 0.18)
    return jnp.clip(array, -most, most).astype(held_as)


def setup_inputs(seed: int = 0) -> dict:
    key_of = jax.random.split(jax.random.key(seed), 7)
    velocity = normal_values(key_of[0], (NX, NY, NZ), 4.0, 24.0, ((0, 16), (1, 2)), jnp.float32)
    viscosity = jnp.clip(jnp.exp(math.log(8000.0) - 2.0794415 * jax.random.uniform(key_of[1], (NX,), jnp.float32) ** levels(key_of[1], (NX,), ((0, 16),), -0.2, 0.2)), 1000.0, 8000.0)
    marker_forces = normal_values(key_of[2], (NBLK, MB), 3.0, 18.0, ((0, 32),))
    spread_weights = normal_values(key_of[3], (NBLK, MB, TILE), MB ** -0.5, 1.5, ((0, 32),))
    block_owner_keys = jax.random.split(jax.random.fold_in(key_of[4], 1), NBLK // BLK_DEV)
    block_owner_turns = jax.random.permutation(jax.random.fold_in(key_of[4], 3), NBLK // BLK_DEV)
    block_owner = jax.vmap(lambda own, number: assign_block(jax.random.fold_in(key_of[4], 2), own, number, BLK_DEV, DEVICES, 1, CAP, 2))(block_owner_keys, block_owner_turns).reshape((NBLK, 1))
    tile_slot = plant(jax.random.randint(key_of[5], (NBLK,), 0, CY * (CZ // SEG)), jax.random.fold_in(key_of[5], 1), 0, (CY * (CZ // SEG)) - 1).astype(jnp.int32)
    return {"velocity": velocity, "viscosity": viscosity, "marker_forces": marker_forces, "spread_weights": spread_weights, "block_owner": block_owner, "tile_slot": tile_slot}


def spread_one(pair):
    return jnp.einsum('bm,bmt->bt', pair[0], pair[1].astype(jnp.float32))

def reference(velocity, viscosity, marker_forces, spread_weights, block_owner, tile_slot):
    forces_dev = marker_forces.reshape(DEVICES, BLK_DEV, MB).astype(jnp.float32)
    weights_dev = spread_weights.reshape(DEVICES, BLK_DEV, MB, TILE)
    tile_values = lax.map(spread_one, (forces_dev, weights_dev))
    rounded = lax.optimization_barrier(tile_values.astype(jnp.bfloat16)).astype(jnp.float32)
    rounded = rounded.reshape(NBLK, CX, SEG)
    owner_dev = block_owner[:, 0]
    owner_x = owner_dev // N_GY
    owner_y = owner_dev % N_GY
    row_y = owner_y * CY + tile_slot // (CZ // SEG)
    seg_z = tile_slot % (CZ // SEG)
    force_field = jnp.zeros((N_GX, CX, NY, CZ // SEG, SEG), jnp.float32)
    force_field = force_field.at[owner_x, :, row_y, seg_z, :].add(rounded)
    right_side = velocity.reshape(NX, NY * NZ) + force_field.reshape(NX, NY * NZ)
    below_all = (-viscosity).at[0].set(0.0)
    above_all = (-viscosity).at[NX - 1].set(0.0)
    main_all = 1.0 + 2.0 * viscosity
    solved = lax.linalg.tridiagonal_solve(below_all, main_all, above_all, right_side)
    return solved.reshape(NX, NY, NZ)
```

```python
import functools

import jax
import jax.numpy as jnp
from jax import lax
from jax.experimental import pallas as pl
from jax.experimental.pallas import tpu as pltpu
from jax.sharding import PartitionSpec as P

F32 = jnp.float32
BF16 = jnp.bfloat16
BASE = 256
LANES = 128
VISC_LANE = 64
TOP = 32767.0
TINY = 1e-30


def iota(shape, axis):
    return lax.broadcasted_iota(jnp.int32, shape, axis)


def nt_dot(a, b):
    return lax.dot_general(a, b, (((1,), (1,)), ((), ())), preferred_element_type=F32)


def tn_dot(a, b):
    return lax.dot_general(a, b, (((0,), (0,)), ((), ())), preferred_element_type=F32)


def factor(visc):
    inverse, ratio = [], []
    for x in range(len(visc) - 1):
        pivot = 1.0 + 2.0 * visc[x]
        if x:
            pivot = pivot - visc[x] * ratio[-1]
        inverse.append(1.0 / pivot)
        ratio.append(visc[x] * inverse[-1])
    return inverse, ratio


def spikes(inverse, ratio):
    count = len(inverse)
    left = [inverse[0]]
    for x in range(1, count):
        left.append(ratio[x] * left[-1])
    for x in range(count - 2, -1, -1):
        left[x] = left[x] + ratio[x] * left[x + 1]
    right = [inverse[-1]]
    for x in range(count - 2, -1, -1):
        right.append(ratio[x] * right[-1])
    return left, right[::-1]


def end_weights(visc, inverse, ratio):
    count = len(inverse)
    last, run = [], visc[-1]
    for x in range(count - 1, -1, -1):
        last.append(run * inverse[x])
        run = run * ratio[x]
    reach = [jnp.ones_like(inverse[0])]
    for x in range(count - 1):
        reach.append(reach[-1] * ratio[x])
    first, total = [], None
    for x in range(count - 1, -1, -1):
        total = reach[x] if total is None else reach[x] + ratio[x + 1] * total
        first.append(visc[0] * inverse[x] * total)
    return last[::-1], first[::-1]


def couple(visc, stride, out_ref):
    rows, lanes = visc[0].shape
    count = rows // stride
    inverse, ratio = factor(visc)
    left, right = spikes(inverse, ratio)
    row = iota((rows, lanes), 0)

    def following(value):
        moved = jnp.concatenate([value[stride:], value[:stride]], axis=0)
        return jnp.where(row >= rows - stride, 0.0, moved)

    sep, inner, first = visc[-1], visc[-2], visc[0]
    lower = jnp.where(row >= stride, -sep * first * left[-1], 0.0)
    center = 1.0 + 2.0 * sep - sep * inner * right[-1] - sep * following(first * left[0])
    upper = -sep * following(inner * right[0])
    final_rows = row >= rows - stride
    held = jnp.where(final_rows, 0.0, sep / jnp.where(final_rows, 1.0, following(first)))
    previous = jnp.zeros((1, lanes), F32)
    for d in range(count):
        at = slice(d * stride, d * stride + 1)
        pivot = center[at] - lower[at] * previous
        inv = 1.0 / pivot
        previous = upper[at] * inv
        out_ref[0, d : d + 1, :] = inv
        out_ref[1, d : d + 1, :] = previous
        out_ref[2, d : d + 1, :] = lower[at]
        out_ref[3, d : d + 1, :] = held[at]


def partner(me, k, count, sign=1):
    if count & (count - 1):
        return lax.rem(me + count + sign * k, count)
    total, bit = 0, 1
    while bit < count:
        total = total + bit * lax.rem(lax.rem(me // bit, 2) + lax.rem(k // bit, 2), 2)
        bit *= 2
    return total


def peak(values):
    most = jnp.abs(values[0])
    for value in values[1:]:
        most = jnp.maximum(most, jnp.abs(value))
    return jnp.maximum(jnp.max(most, axis=0, keepdims=True), TINY)


def pack(high, low, inverse):
    high = jnp.round(high * inverse).astype(jnp.int32)
    low = jnp.round(low * inverse).astype(jnp.int32)
    return high * 65536 + low


def unpack(code, scale):
    low = (code << 16) >> 16
    high = (code - low) >> 16
    return high.astype(F32) * scale, low.astype(F32) * scale


def step_kernel(
    count_x, count_y, capacity, chunks,
    visc_hbm, forces_hbm, weights_hbm, owner_hbm, slot_hbm, velocity_hbm,
    inner_ref, back_ref, back_scale_ref, mix_ref,
    visc_ref, forces_ref, owner_ref, slot_ref, weights_ref, velocity_ref,
    spread_ref, outgoing_ref, tiles_ref, meta_ref, metas_ref, place_ref, tile_ends_ref, ends_ref,
    local_ref, weight_ref, couple_ref, code_ref, code_scale_ref, sides_ref, sides_scale_ref,
    solved_ref, home_ref, home_scale_ref, rhs_ref, flat_ref,
    own, wsem, tile_send, tile_recv, meta_send, meta_recv,
    code_send, code_recv, cscale_send, cscale_recv, home_send, home_recv, hscale_send, hscale_recv,
):
    devices = count_x * count_y
    cells_x, rows_y, cells_z = velocity_ref.shape
    markers, blocks = forces_ref.shape
    cells = outgoing_ref.shape[2]
    wide = blocks * markers
    rows = devices * capacity
    share = code_ref.shape[1]
    width = cells // chunks
    segments = cells_z // LANES
    last = cells_x - 1
    gx, gy = lax.axis_index("gx"), lax.axis_index("gy")
    me = gx * count_y + gy

    def device(i):
        peer = partner(me, i, devices)
        return (peer // count_y, lax.rem(peer, count_y))

    def loop(first, end, body, unroll=1):
        def step(i, carry):
            body(i)
            return carry

        lax.fori_loop(first, end, step, 0, unroll=unroll)

    barrier = pltpu.get_barrier_semaphore()

    def greet(i):
        pl.semaphore_signal(
            barrier, inc=1, device_id=device(i), device_id_type=pl.DeviceIdType.MESH
        )

    small = [
        pltpu.make_async_copy(source, target, own.at[k])
        for k, (source, target) in enumerate(
            ((owner_hbm, owner_ref), (forces_hbm, forces_ref), (slot_hbm, slot_ref), (visc_hbm, visc_ref))
        )
    ]
    for copy in small:
        copy.start()

    def weight_copy(c):
        at = pl.ds(pl.multiple_of(c * width, width), width)
        return pltpu.make_async_copy(weights_hbm.at[:, :, at], weights_ref.at[c], wsem.at[c])

    loop(0, chunks, lambda c: weight_copy(c).start())
    velocity_copy = pltpu.make_async_copy(velocity_hbm, velocity_ref, own.at[4])
    velocity_copy.start()
    loop(1, devices, greet)
    for copy in small:
        copy.wait()

    owner = owner_ref[...]
    matches = (iota((devices, blocks), 0) == owner).astype(BF16)
    earlier = (iota((blocks, blocks), 0) < iota((blocks, blocks), 1)).astype(BF16)
    counts = jnp.dot(matches, earlier, preferred_element_type=F32)
    rank = jnp.sum(counts * matches.astype(F32), axis=0, keepdims=True).astype(jnp.int32)
    target = owner * capacity + rank
    select = (iota((rows, blocks), 0) == target).astype(BF16)
    choose = (iota((markers, wide), 1) % markers == iota((markers, wide), 0)).astype(BF16)
    tiled = tn_dot(forces_ref[...], choose)
    offset = iota((blocks, wide), 1) - iota((blocks, wide), 0) * markers
    spread = jnp.where((offset >= 0) & (offset < markers), tiled, 0.0).astype(BF16)
    spread_ref[...] = jnp.dot(select, spread, preferred_element_type=F32).astype(BF16)

    number = slot_ref[...] + 1
    high = number // BASE
    ranked = iota((LANES, blocks), 0) == rank
    digits = [jnp.where(ranked, d, 0).astype(F32).astype(BF16) for d in (high, number - high * BASE)]
    meta = nt_dot(matches, digits[0]) * BASE + nt_dot(matches, digits[1])
    lane = iota((1, LANES), 1)
    viscous = jnp.zeros((1, LANES), F32)
    for x in range(cells_x):
        viscous = jnp.where(lane == VISC_LANE + x, visc_ref[x], viscous)
    meta = meta + viscous
    for d in range(devices):
        meta_ref[d] = meta[d : d + 1]

    def spread_chunk(c):
        weight_copy(c).wait()
        at = pl.ds(pl.multiple_of(c * width, width), width)
        out = jnp.dot(
            spread_ref[...], weights_ref[c].reshape(wide, width), preferred_element_type=F32
        )
        if capacity % 8 == 0:
            outgoing_ref[:, :, at] = out.reshape(devices, capacity, width).astype(BF16)
        else:
            for d in range(devices):
                outgoing_ref[d, :, at] = out[d * capacity : (d + 1) * capacity].astype(BF16)

    loop(0, chunks, spread_chunk)

    def remote(source, target, sends, receives, i, peer):
        return pltpu.make_async_remote_copy(
            src_ref=source,
            dst_ref=target,
            send_sem=sends.at[i],
            recv_sem=receives.at[i],
            device_id=peer,
            device_id_type=pl.DeviceIdType.MESH,
        )

    def tile_copy(i, slot):
        peer = partner(me, i, devices)
        return remote(outgoing_ref.at[peer], tiles_ref.at[slot], tile_send, tile_recv, i, device(i))

    def meta_copy(i, slot):
        peer = partner(me, i, devices)
        return remote(meta_ref.at[peer], metas_ref.at[slot], meta_send, meta_recv, i, device(i))

    def came(i):
        return partner(me, i, devices, -1)

    pl.semaphore_wait(barrier, devices - 1)
    loop(1, devices, lambda i: meta_copy(i, me).start())
    loop(1, devices, lambda i: tile_copy(i, me).start())
    tiles_ref[me] = outgoing_ref[me]
    metas_ref[me] = meta_ref[me]

    visc = [jnp.full((8, LANES), visc_ref[x], F32) for x in range(cells_x)]
    inverse, ratio = factor(visc)
    for x in range(last):
        local_ref[x] = inverse[x]
        local_ref[cells_x + x] = ratio[x]
    to_last, to_first = end_weights(visc, inverse, ratio)
    for x in range(last):
        weight_ref[x] = to_last[x]
        weight_ref[cells_x + x] = to_first[x]
    left, right = spikes(inverse, ratio)
    for x in range(last):
        mix_ref[x] = visc[0] * left[x]
        mix_ref[last + x] = visc[last - 1] * right[x]

    def ends_of(side):
        value = side(0)
        high, low = value * weight_ref[0], value * weight_ref[cells_x]
        for x in range(1, last):
            value = side(x)
            high = high + value * weight_ref[x]
            low = low + value * weight_ref[cells_x + x]
        return high + side(last), low

    velocity_copy.wait()

    def velocity_ends(i):
        at = pl.ds(pl.multiple_of(i * 8, 8), 8)
        for s in range(segments):
            lanes = slice(s * LANES, (s + 1) * LANES)
            high, low = ends_of(lambda x: velocity_ref[x, at, lanes])
            ends_ref[0, at, lanes] = high
            ends_ref[1, at, lanes] = low

    loop(0, rows_y // 8, velocity_ends)

    loop(1, devices, lambda i: meta_copy(i, came(i)).wait())
    metas = jnp.concatenate([metas_ref[d] for d in range(devices)], axis=0)
    couple(
        [
            jnp.broadcast_to(metas[:, VISC_LANE + x : VISC_LANE + x + 1], (devices, LANES))
            for x in range(cells_x)
        ],
        count_y,
        couple_ref,
    )
    lane = iota((devices, LANES), 1)
    numbers = jnp.where(lane < capacity, metas, 0.0).astype(jnp.int32)
    high = numbers // BASE
    expand = (iota((LANES, rows), 1) % capacity == iota((LANES, rows), 0)).astype(BF16)
    number = jnp.zeros((devices, rows), F32)
    for digit, base in ((high, float(BASE)), (numbers - high * BASE, 1.0)):
        number = number + base * jnp.dot(
            digit.astype(F32).astype(BF16), expand, preferred_element_type=F32
        )
    offset = iota((devices, rows), 1) - iota((devices, rows), 0) * capacity
    number = jnp.where((offset >= 0) & (offset < capacity), number, 0.0)
    number = jnp.sum(number, axis=0, keepdims=True).astype(jnp.int32) - 1
    for s in range(segments):
        place_ref[s] = (iota((rows_y, rows), 0) * segments + s == number).astype(BF16)

    def tile_ends(slot):
        at = pl.ds(pl.multiple_of(slot * capacity, capacity), capacity)
        high, low = ends_of(lambda x: tiles_ref[slot, :, x * LANES : (x + 1) * LANES].astype(F32))
        tile_ends_ref[at, :LANES] = high
        tile_ends_ref[at, LANES:] = low

    def flatten():
        if capacity % 8 == 0:
            flat_ref[...] = tiles_ref[...].astype(F32).reshape(rows, cells).astype(BF16)
        else:
            parts = [tiles_ref[d].astype(F32) for d in range(devices)]
            flat_ref[...] = jnp.concatenate(parts, axis=0).astype(BF16)

    if capacity % 8 == 0:
        tile_ends(me)

        def arrive(i):
            tile_copy(i, came(i)).wait_recv()
            tile_ends(came(i))

        loop(1, devices, arrive)
    else:
        loop(1, devices, lambda i: tile_copy(i, came(i)).wait_recv())
        flatten()

        def flat_ends(i):
            at = pl.ds(pl.multiple_of(i * 8, 8), 8)
            high, low = ends_of(lambda x: flat_ref[at, x * LANES : (x + 1) * LANES].astype(F32))
            tile_ends_ref[at, :LANES] = high
            tile_ends_ref[at, LANES:] = low

        loop(0, rows // 8, flat_ends)

    found = tile_ends_ref[...]
    coarse = found.astype(BF16)
    fine = (found - coarse.astype(F32)).astype(BF16)
    for s in range(segments):
        lanes = slice(s * LANES, (s + 1) * LANES)
        placed = jnp.dot(place_ref[s], coarse, preferred_element_type=F32)
        placed = placed + jnp.dot(place_ref[s], fine, preferred_element_type=F32)
        ends_ref[0, :, lanes] = ends_ref[0, :, lanes] + placed[:, :LANES]
        ends_ref[1, :, lanes] = ends_ref[1, :, lanes] + placed[:, LANES:]

    def line_copy(source, target, sends, receives, i, slot):
        peer = partner(gx, i, count_x)
        return remote(source.at[peer], target.at[slot], sends, receives, i, (peer, gy))

    outward = ((code_ref, sides_ref, code_send, code_recv), (code_scale_ref, sides_scale_ref, cscale_send, cscale_recv))
    homeward = ((home_ref, back_ref, home_send, home_recv), (home_scale_ref, back_scale_ref, hscale_send, hscale_recv))

    def start(groups, i):
        for group in groups:
            line_copy(*group, i, gx).start()

    def finish(groups, i):
        for group in groups:
            line_copy(*group, i, partner(gx, i, count_x, -1)).wait()

    def code_rows(i):
        at = pl.ds(pl.multiple_of(i * 8, 8), 8)
        pairs = []
        for s in range(segments):
            lanes = slice(s * LANES, (s + 1) * LANES)
            pairs.append((ends_ref[0, at, lanes], ends_ref[1, at, lanes]))
        most = peak([value for pair in pairs for value in pair])
        inverse = TOP / most
        codes = [pack(high, low, inverse) for high, low in pairs]
        scale = most * (1.0 / TOP)
        return codes, scale

    if share % 8 == 0:

        def code_peer(peer):
            most = None
            for k in range(share // 8):
                at = pl.ds(pl.multiple_of(peer * share + k * 8, 8), 8)
                top = peak([ends_ref[w, at, s * LANES : (s + 1) * LANES] for s in range(segments) for w in (0, 1)])
                most = top if most is None else jnp.maximum(most, top)
            inverse = TOP / most
            code_scale_ref[peer] = most * (1.0 / TOP)
            for k in range(share // 8):
                at = pl.ds(pl.multiple_of(peer * share + k * 8, 8), 8)
                for s in range(segments):
                    lanes = slice(s * LANES, (s + 1) * LANES)
                    code_ref[peer, k * 8 : (k + 1) * 8, lanes] = pack(
                        ends_ref[0, at, lanes], ends_ref[1, at, lanes], inverse
                    )

        def code_and_start(i):
            code_peer(partner(gx, i, count_x))
            start(outward, i)

        loop(1, count_x, code_and_start)
        code_peer(gx)
    else:
        group = 8 // share
        for i in range(rows_y // 8):
            codes, scale = code_rows(i)
            for k in range(group):
                code_scale_ref[i * group + k] = scale
                for s in range(segments):
                    code_ref[i * group + k, :, s * LANES : (s + 1) * LANES] = codes[s][k * share : (k + 1) * share]
        loop(1, count_x, lambda i: start(outward, i))
    sides_ref[gx] = code_ref[gx]
    sides_scale_ref[gx] = code_scale_ref[gx]

    if capacity % 8 == 0:
        flatten()
    for s in range(segments):
        lanes = slice(s * LANES, (s + 1) * LANES)
        rhs_ref[...] = jnp.dot(place_ref[s], flat_ref[:, : last * LANES], preferred_element_type=F32)

        def solve(i):
            at = pl.ds(pl.multiple_of(i * 8, 8), 8)
            values = []
            for x in range(last):
                side = velocity_ref[x, at, lanes] + rhs_ref[at, x * LANES : (x + 1) * LANES]
                side = side * local_ref[x]
                values.append(side + local_ref[cells_x + x] * values[-1] if x else side)
            value = values[-1]
            inner_ref[last - 1, at, lanes] = value
            for x in range(last - 2, -1, -1):
                value = values[x] + local_ref[cells_x + x] * value
                inner_ref[x, at, lanes] = value

        loop(0, rows_y // 8, solve, unroll=2)

    loop(1, count_x, lambda i: finish(outward, i))

    most = jnp.full((share, LANES), 0.0, F32)
    for s in range(segments):
        lanes = slice(s * LANES, (s + 1) * LANES)
        values = []
        after = None
        sides = [unpack(sides_ref[d, :, lanes], sides_scale_ref[d]) for d in range(count_x)]
        for d in range(count_x):
            side = sides[d][0]
            if d + 1 < count_x:
                side = side + couple_ref[3, d : d + 1, :] * sides[d + 1][1]
            if d:
                side = side - couple_ref[2, d : d + 1, :] * values[-1]
            values.append(side * couple_ref[0, d : d + 1, :])
        value = values[-1]
        solved_ref[count_x - 1, :, lanes] = value
        most = jnp.maximum(most, jnp.abs(value))
        for d in range(count_x - 2, -1, -1):
            value = values[d] - couple_ref[1, d : d + 1, :] * value
            solved_ref[d, :, lanes] = value
            most = jnp.maximum(most, jnp.abs(value))

    most = jnp.maximum(jnp.max(most, axis=0, keepdims=True), TINY)
    inverse = TOP / most
    scale = most * (1.0 / TOP)

    def home_code(d):
        home_scale_ref[d] = scale
        before = jnp.where(d > 0, 1.0, 0.0)
        for s in range(segments):
            lanes = slice(s * LANES, (s + 1) * LANES)
            home_ref[d, :, lanes] = pack(
                solved_ref[d, :, lanes], solved_ref[jnp.maximum(d - 1, 0), :, lanes] * before, inverse
            )

    def home_and_start(i):
        home_code(partner(gx, i, count_x))
        start(homeward, i)

    loop(1, count_x, home_and_start)
    home_code(gx)
    back_ref[gx] = home_ref[gx]
    back_scale_ref[gx] = home_scale_ref[gx]
    loop(1, devices, lambda i: tile_copy(i, came(i)).wait_send())
    loop(1, count_x, lambda i: finish(homeward, i))


def step(viscosity, forces, weights, owner, slots, velocity, grid_x, grid_y, capacity):
    cells_x, cells_y, cells_z = velocity.shape
    blocks, markers, cells = weights.shape
    devices = grid_x * grid_y
    rows = devices * capacity
    share = cells_y // grid_x
    chunks = 4
    dma = pltpu.SemaphoreType.DMA
    vmem = pltpu.VMEM
    anywhere = pl.BlockSpec(memory_space=pl.ANY)
    whole = pl.BlockSpec(memory_space=pltpu.VMEM)
    line = (grid_x, share, cells_z)
    line_scale = (grid_x, 1, LANES)

    def keep(value):
        return pltpu.with_memory_space_constraint(value, pltpu.HBM)

    return pl.pallas_call(
        functools.partial(step_kernel, grid_x, grid_y, capacity, chunks),
        out_shape=(
            jax.ShapeDtypeStruct((cells_x - 1, cells_y, cells_z), F32),
            jax.ShapeDtypeStruct(line, jnp.int32),
            jax.ShapeDtypeStruct(line_scale, F32),
            jax.ShapeDtypeStruct((2 * (cells_x - 1), 8, LANES), F32),
        ),
        in_specs=[anywhere] * 6,
        out_specs=(whole,) * 4,
        scratch_shapes=[
            pltpu.SMEM((cells_x,), F32),
            vmem((markers, blocks), BF16),
            vmem((1, blocks), jnp.int32),
            vmem((1, blocks), jnp.int32),
            vmem((chunks, blocks, markers, cells // chunks), BF16),
            vmem((cells_x, cells_y, cells_z), F32),
            vmem((rows, blocks * markers), BF16),
            vmem((devices, capacity, cells), BF16),
            vmem((devices, capacity, cells), BF16),
            vmem((devices, 1, LANES), F32),
            vmem((devices, 1, LANES), F32),
            vmem((cells_z // LANES, cells_y, rows), BF16),
            vmem((rows, 2 * LANES), F32),
            vmem((2, cells_y, cells_z), F32),
            vmem((2 * cells_x, 8, LANES), F32),
            vmem((2 * cells_x, 8, LANES), F32),
            vmem((4, grid_x, LANES), F32),
            vmem(line, jnp.int32),
            vmem(line_scale, F32),
            vmem(line, jnp.int32),
            vmem(line_scale, F32),
            vmem(line, F32),
            vmem(line, jnp.int32),
            vmem(line_scale, F32),
            vmem((cells_y, (cells_x - 1) * LANES), F32),
            vmem((rows, cells), BF16),
            dma((5,)),
            dma((chunks,)),
            dma((devices,)),
            dma((devices,)),
            dma((devices,)),
            dma((devices,)),
        ]
        + [dma((grid_x,))] * 8,
        compiler_params=pltpu.CompilerParams(
            collective_id=0, has_side_effects=True, vmem_limit_bytes=40 << 20
        ),
    )(
        keep(viscosity), keep(forces), keep(weights), keep(owner), keep(slots), keep(velocity)
    )


def rows_of(ref, i):
    rows = ref.shape[1]
    if rows % 8 == 0:
        start = pl.multiple_of(lax.rem(i * 8, rows), 8)
        return lambda lane: ref[i * 8 // rows, pl.ds(start, 8), lane]
    share = 8 // rows
    return lambda lane: jnp.concatenate([ref[i * share + k, :, lane] for k in range(share)], axis=0)


def scale_of(ref, i, rows):
    if rows % 8 == 0:
        return ref[i * 8 // rows]
    share = 8 // rows
    parts = [jnp.broadcast_to(ref[i * share + k], (rows, LANES)) for k in range(share)]
    return jnp.concatenate(parts, axis=0)


def final_kernel(inner_ref, back_ref, scale_ref, mix_ref, out_ref):
    count, rows_y, cells_z = inner_ref.shape

    def chunk(i, carry):
        at = pl.ds(pl.multiple_of(i * 8, 8), 8)
        codes = rows_of(back_ref, i)
        scale = scale_of(scale_ref, i, back_ref.shape[1])
        for c in range(cells_z // LANES):
            lane = slice(c * LANES, (c + 1) * LANES)
            last, before = unpack(codes(lane), scale)
            for x in range(count):
                out_ref[x, at, lane] = (
                    inner_ref[x, at, lane] + mix_ref[x] * before + mix_ref[count + x] * last
                )
            out_ref[count, at, lane] = last
        return carry

    lax.fori_loop(0, rows_y // 8, chunk, 0)


def final(inner, back, scale, mix):
    count, cells_y, cells_z = inner.shape
    parts = 4
    rows = cells_y // parts
    peers = back.shape[0] // parts
    return pl.pallas_call(
        final_kernel,
        out_shape=jax.ShapeDtypeStruct((count + 1, cells_y, cells_z), F32),
        grid=(parts,),
        in_specs=[
            pl.BlockSpec((count, rows, cells_z), lambda i: (0, i, 0)),
            pl.BlockSpec((peers,) + back.shape[1:], lambda i: (i, 0, 0)),
            pl.BlockSpec((peers,) + scale.shape[1:], lambda i: (i, 0, 0)),
            pl.BlockSpec(mix.shape, lambda i: (0, 0, 0)),
        ],
        out_specs=pl.BlockSpec((count + 1, rows, cells_z), lambda i: (0, i, 0)),
        compiler_params=pltpu.CompilerParams(vmem_limit_bytes=24 << 20),
    )(inner, back, scale, mix)


def per_device(velocity, viscosity, marker_forces, spread_weights, block_owner, tile_slot):
    grid_x, grid_y = lax.axis_size("gx"), lax.axis_size("gy")
    blocks = spread_weights.shape[0]
    capacity = max(2, 2 * blocks // (grid_x * grid_y))
    inner, back, scale, mix = step(
        viscosity,
        marker_forces.T,
        spread_weights,
        block_owner.reshape(1, blocks),
        tile_slot.reshape(1, blocks),
        velocity,
        grid_x,
        grid_y,
        capacity,
    )
    return final(inner, back, scale, mix)


def solution(mesh):
    placed = (
        P("gx", "gy", None),
        P("gx"),
        P(("gx", "gy"), None),
        P(("gx", "gy"), None, None),
        P(("gx", "gy"), None),
        P(("gx", "gy")),
    )
    return jax.shard_map(
        per_device, mesh=mesh, in_specs=placed, out_specs=P("gx", "gy", None), check_vma=False
    )
```

```python
import functools

import jax
import jax.numpy as jnp
from jax import lax
from jax.experimental import pallas as pl
from jax.experimental.pallas import tpu as pltpu
from jax.sharding import PartitionSpec as P

F32 = jnp.float32
BF16 = jnp.bfloat16
BASE = 256
LANES = 128
VISC_LANE = 64
TOP = 32767.0
TINY = 1e-30


def iota(shape, axis):
    return lax.broadcasted_iota(jnp.int32, shape, axis)


def nt_dot(a, b):
    return lax.dot_general(a, b, (((1,), (1,)), ((), ())), preferred_element_type=F32)


def tn_dot(a, b):
    return lax.dot_general(a, b, (((0,), (0,)), ((), ())), preferred_element_type=F32)


def factor(visc):
    inverse, ratio = [], []
    for x in range(len(visc) - 1):
        pivot = 1.0 + 2.0 * visc[x]
        if x:
            pivot = pivot - visc[x] * ratio[-1]
        inverse.append(1.0 / pivot)
        ratio.append(visc[x] * inverse[-1])
    return inverse, ratio


def spikes(inverse, ratio):
    count = len(inverse)
    left = [inverse[0]]
    for x in range(1, count):
        left.append(ratio[x] * left[-1])
    for x in range(count - 2, -1, -1):
        left[x] = left[x] + ratio[x] * left[x + 1]
    right = [inverse[-1]]
    for x in range(count - 2, -1, -1):
        right.append(ratio[x] * right[-1])
    return left, right[::-1]


def end_weights(visc, inverse, ratio):
    count = len(inverse)
    last, run = [], visc[-1]
    for x in range(count - 1, -1, -1):
        last.append(run * inverse[x])
        run = run * ratio[x]
    reach = [jnp.ones_like(inverse[0])]
    for x in range(count - 1):
        reach.append(reach[-1] * ratio[x])
    first, total = [], None
    for x in range(count - 1, -1, -1):
        total = reach[x] if total is None else reach[x] + ratio[x + 1] * total
        first.append(visc[0] * inverse[x] * total)
    return last[::-1], first[::-1]


def couple(visc, stride, out_ref):
    rows, lanes = visc[0].shape
    count = rows // stride
    inverse, ratio = factor(visc)
    left, right = spikes(inverse, ratio)
    row = iota((rows, lanes), 0)

    def following(value):
        moved = jnp.concatenate([value[stride:], value[:stride]], axis=0)
        return jnp.where(row >= rows - stride, 0.0, moved)

    sep, inner, first = visc[-1], visc[-2], visc[0]
    lower = jnp.where(row >= stride, -sep * first * left[-1], 0.0)
    center = 1.0 + 2.0 * sep - sep * inner * right[-1] - sep * following(first * left[0])
    upper = -sep * following(inner * right[0])
    final_rows = row >= rows - stride
    held = jnp.where(final_rows, 0.0, sep / jnp.where(final_rows, 1.0, following(first)))
    previous = jnp.zeros((1, lanes), F32)
    for d in range(count):
        at = slice(d * stride, d * stride + 1)
        pivot = center[at] - lower[at] * previous
        inv = 1.0 / pivot
        previous = upper[at] * inv
        out_ref[0, d : d + 1, :] = inv
        out_ref[1, d : d + 1, :] = previous
        out_ref[2, d : d + 1, :] = lower[at]
        out_ref[3, d : d + 1, :] = held[at]


def peers(me, count):
    if count & (count - 1):
        return (lambda k: lax.rem(me + k, count)), (lambda k: lax.rem(me + count - k, count))
    steps, bit = [], 1
    while bit < count:
        steps.append(bit - 2 * bit * lax.rem(me // bit, 2))
        bit *= 2

    def peer(k):
        moved = me
        for n, step in enumerate(steps):
            if k >> n & 1:
                moved = moved + step
        return moved

    return peer, peer


def peak(values):
    most = jnp.abs(values[0])
    for value in values[1:]:
        most = jnp.maximum(most, jnp.abs(value))
    return jnp.maximum(jnp.max(most, axis=0, keepdims=True), TINY)


def pack(high, low, inverse):
    high = jnp.round(high * inverse).astype(jnp.int32)
    low = jnp.round(low * inverse).astype(jnp.int32)
    return high * 65536 + low


def unpack(code, scale):
    low = (code << 16) >> 16
    high = (code - low) >> 16
    return high.astype(F32) * scale, low.astype(F32) * scale


def step_kernel(
    count_x, count_y, capacity, chunks,
    visc_hbm, forces_hbm, weights_hbm, owner_hbm, slot_hbm, velocity_hbm,
    inner_ref, back_ref, back_scale_ref, mix_ref,
    visc_ref, forces_ref, owner_ref, slot_ref, weights_ref, velocity_ref,
    spread_ref, outgoing_ref, tiles_ref, meta_ref, metas_ref, place_ref, tile_ends_ref, ends_ref,
    local_ref, weight_ref, couple_ref, code_ref, code_scale_ref, sides_ref, sides_scale_ref,
    solved_ref, home_ref, home_scale_ref, rhs_ref, flat_ref,
    own, wsem, tile_send, tile_recv, meta_send, meta_recv,
    code_send, code_recv, cscale_send, cscale_recv, home_send, home_recv, hscale_send, hscale_recv,
):
    devices = count_x * count_y
    cells_x, rows_y, cells_z = velocity_ref.shape
    markers, blocks = forces_ref.shape
    cells = outgoing_ref.shape[2]
    wide = blocks * markers
    rows = devices * capacity
    share = code_ref.shape[1]
    width = cells // chunks
    segments = cells_z // LANES
    last = cells_x - 1
    gx, gy = lax.axis_index("gx"), lax.axis_index("gy")
    me = gx * count_y + gy

    to_x, from_x = peers(gx, count_x)
    to_y, from_y = peers(gy, count_y)

    def device(i):
        return (to_x(i // count_y), to_y(i % count_y))

    def index(i):
        px, py = device(i)
        return px * count_y + py

    def came(i):
        return from_x(i // count_y) * count_y + from_y(i % count_y)

    def loop(first, end, body, unroll=1):
        def step(i, carry):
            body(i)
            return carry

        lax.fori_loop(first, end, step, 0, unroll=unroll)

    barrier = pltpu.get_barrier_semaphore()

    for i in range(1, devices):
        pl.semaphore_signal(
            barrier, inc=1, device_id=device(i), device_id_type=pl.DeviceIdType.MESH
        )

    small = [
        pltpu.make_async_copy(source, target, own.at[k])
        for k, (source, target) in enumerate(
            ((owner_hbm, owner_ref), (forces_hbm, forces_ref), (slot_hbm, slot_ref), (visc_hbm, visc_ref))
        )
    ]
    for copy in small:
        copy.start()

    def weight_copy(c):
        at = pl.ds(pl.multiple_of(c * width, width), width)
        return pltpu.make_async_copy(weights_hbm.at[:, :, at], weights_ref.at[c], wsem.at[c])

    loop(0, chunks, lambda c: weight_copy(c).start())
    velocity_copy = pltpu.make_async_copy(velocity_hbm, velocity_ref, own.at[4])
    velocity_copy.start()
    for copy in small:
        copy.wait()

    owner = owner_ref[...]
    matches = (iota((devices, blocks), 0) == owner).astype(BF16)
    earlier = (iota((blocks, blocks), 0) < iota((blocks, blocks), 1)).astype(BF16)
    counts = jnp.dot(matches, earlier, preferred_element_type=F32)
    rank = jnp.sum(counts * matches.astype(F32), axis=0, keepdims=True).astype(jnp.int32)
    target = owner * capacity + rank
    select = (iota((rows, blocks), 0) == target).astype(BF16)
    choose = (iota((markers, wide), 1) % markers == iota((markers, wide), 0)).astype(BF16)
    tiled = tn_dot(forces_ref[...], choose)
    offset = iota((blocks, wide), 1) - iota((blocks, wide), 0) * markers
    spread = jnp.where((offset >= 0) & (offset < markers), tiled, 0.0).astype(BF16)
    spread_ref[...] = jnp.dot(select, spread, preferred_element_type=F32).astype(BF16)

    number = slot_ref[...] + 1
    high = number // BASE
    ranked = iota((LANES, blocks), 0) == rank
    digits = [jnp.where(ranked, d, 0).astype(F32).astype(BF16) for d in (high, number - high * BASE)]
    meta = nt_dot(matches, digits[0]) * BASE + nt_dot(matches, digits[1])
    lane = iota((1, LANES), 1)
    viscous = jnp.zeros((1, LANES), F32)
    for x in range(cells_x):
        viscous = jnp.where(lane == VISC_LANE + x, visc_ref[x], viscous)
    meta = meta + viscous
    for d in range(devices):
        meta_ref[d] = meta[d : d + 1]

    def spread_chunk(c):
        weight_copy(c).wait()
        at = pl.ds(pl.multiple_of(c * width, width), width)
        out = jnp.dot(
            spread_ref[...], weights_ref[c].reshape(wide, width), preferred_element_type=F32
        )
        if capacity % 8 == 0:
            outgoing_ref[:, :, at] = out.reshape(devices, capacity, width).astype(BF16)
        else:
            for d in range(devices):
                outgoing_ref[d, :, at] = out[d * capacity : (d + 1) * capacity].astype(BF16)

    loop(0, chunks, spread_chunk)

    def remote(source, target, sends, receives, i, peer):
        return pltpu.make_async_remote_copy(
            src_ref=source,
            dst_ref=target,
            send_sem=sends.at[i],
            recv_sem=receives.at[i],
            device_id=peer,
            device_id_type=pl.DeviceIdType.MESH,
        )

    def tile_copy(i, slot):
        peer = index(i)
        return remote(outgoing_ref.at[peer], tiles_ref.at[slot], tile_send, tile_recv, i, device(i))

    def meta_copy(i, slot):
        peer = index(i)
        return remote(meta_ref.at[peer], metas_ref.at[slot], meta_send, meta_recv, i, device(i))

    pl.semaphore_wait(barrier, devices - 1)
    for i in range(1, devices):
        meta_copy(i, me).start()
    for i in range(1, devices):
        tile_copy(i, me).start()
    tiles_ref[me] = outgoing_ref[me]
    metas_ref[me] = meta_ref[me]

    visc = [jnp.full((8, LANES), visc_ref[x], F32) for x in range(cells_x)]
    inverse, ratio = factor(visc)
    for x in range(last):
        local_ref[x] = inverse[x]
        local_ref[cells_x + x] = ratio[x]
    to_last, to_first = end_weights(visc, inverse, ratio)
    for x in range(last):
        weight_ref[x] = to_last[x]
        weight_ref[cells_x + x] = to_first[x]
    left, right = spikes(inverse, ratio)
    for x in range(last):
        mix_ref[x] = visc[0] * left[x]
        mix_ref[last + x] = visc[last - 1] * right[x]

    def ends_of(side):
        value = side(0)
        high, low = value * weight_ref[0], value * weight_ref[cells_x]
        for x in range(1, last):
            value = side(x)
            high = high + value * weight_ref[x]
            low = low + value * weight_ref[cells_x + x]
        return high + side(last), low

    velocity_copy.wait()

    def velocity_ends(i):
        at = pl.ds(pl.multiple_of(i * 8, 8), 8)
        for s in range(segments):
            lanes = slice(s * LANES, (s + 1) * LANES)
            high, low = ends_of(lambda x: velocity_ref[x, at, lanes])
            ends_ref[0, at, lanes] = high
            ends_ref[1, at, lanes] = low

    loop(0, rows_y // 8, velocity_ends)

    for i in range(1, devices):
        meta_copy(i, came(i)).wait()
    metas = jnp.concatenate([metas_ref[d] for d in range(devices)], axis=0)
    couple(
        [
            jnp.broadcast_to(metas[:, VISC_LANE + x : VISC_LANE + x + 1], (devices, LANES))
            for x in range(cells_x)
        ],
        count_y,
        couple_ref,
    )
    lane = iota((devices, LANES), 1)
    numbers = jnp.where(lane < capacity, metas, 0.0).astype(jnp.int32)
    high = numbers // BASE
    expand = (iota((LANES, rows), 1) % capacity == iota((LANES, rows), 0)).astype(BF16)
    number = jnp.zeros((devices, rows), F32)
    for digit, base in ((high, float(BASE)), (numbers - high * BASE, 1.0)):
        number = number + base * jnp.dot(
            digit.astype(F32).astype(BF16), expand, preferred_element_type=F32
        )
    offset = iota((devices, rows), 1) - iota((devices, rows), 0) * capacity
    number = jnp.where((offset >= 0) & (offset < capacity), number, 0.0)
    number = jnp.sum(number, axis=0, keepdims=True).astype(jnp.int32) - 1
    for s in range(segments):
        place_ref[s * rows_y : (s + 1) * rows_y] = (
            iota((rows_y, rows), 0) * segments + s == number
        ).astype(BF16)

    def tile_ends(slot):
        at = pl.ds(pl.multiple_of(slot * capacity, capacity), capacity)
        high, low = ends_of(lambda x: tiles_ref[slot, :, x * LANES : (x + 1) * LANES].astype(F32))
        tile_ends_ref[at, :LANES] = high
        tile_ends_ref[at, LANES:] = low

    def flatten():
        if capacity % 8 == 0:
            flat_ref[...] = tiles_ref[...].astype(F32).reshape(rows, cells).astype(BF16)
        else:
            parts = [tiles_ref[d].astype(F32) for d in range(devices)]
            flat_ref[...] = jnp.concatenate(parts, axis=0).astype(BF16)

    if capacity % 8 == 0:
        tile_ends(me)

        for i in range(1, devices):
            tile_copy(i, came(i)).wait_recv()
            tile_ends(came(i))
    else:
        for i in range(1, devices):
            tile_copy(i, came(i)).wait_recv()
        flatten()

        def flat_ends(i):
            at = pl.ds(pl.multiple_of(i * 8, 8), 8)
            high, low = ends_of(lambda x: flat_ref[at, x * LANES : (x + 1) * LANES].astype(F32))
            tile_ends_ref[at, :LANES] = high
            tile_ends_ref[at, LANES:] = low

        loop(0, rows // 8, flat_ends)

    found = tile_ends_ref[...]
    coarse = found.astype(BF16)
    fine = (found - coarse.astype(F32)).astype(BF16)
    both = jnp.concatenate([coarse, fine], axis=1)
    placed = jnp.dot(place_ref[...], both, preferred_element_type=F32)
    for s in range(segments):
        lanes = slice(s * LANES, (s + 1) * LANES)
        part = placed[s * rows_y : (s + 1) * rows_y]
        for w in (0, 1):
            ends_ref[w, :, lanes] = ends_ref[w, :, lanes] + (
                part[:, w * LANES : (w + 1) * LANES] + part[:, (w + 2) * LANES : (w + 3) * LANES]
            )

    def line_copy(source, target, sends, receives, i, slot):
        peer = to_x(i)
        return remote(source.at[peer], target.at[slot], sends, receives, i, (peer, gy))

    outward = ((code_ref, sides_ref, code_send, code_recv), (code_scale_ref, sides_scale_ref, cscale_send, cscale_recv))
    homeward = ((home_ref, back_ref, home_send, home_recv), (home_scale_ref, back_scale_ref, hscale_send, hscale_recv))

    def start(groups, i):
        for group in groups:
            line_copy(*group, i, gx).start()

    def finish(groups, i):
        for group in groups:
            line_copy(*group, i, from_x(i)).wait()

    def code_rows(i):
        at = pl.ds(pl.multiple_of(i * 8, 8), 8)
        pairs = []
        for s in range(segments):
            lanes = slice(s * LANES, (s + 1) * LANES)
            pairs.append((ends_ref[0, at, lanes], ends_ref[1, at, lanes]))
        most = peak([value for pair in pairs for value in pair])
        inverse = TOP / most
        codes = [pack(high, low, inverse) for high, low in pairs]
        scale = most * (1.0 / TOP)
        return codes, scale

    if share % 8 == 0:

        def code_peer(peer):
            most = None
            for k in range(share // 8):
                at = pl.ds(pl.multiple_of(peer * share + k * 8, 8), 8)
                top = peak([ends_ref[w, at, s * LANES : (s + 1) * LANES] for s in range(segments) for w in (0, 1)])
                most = top if most is None else jnp.maximum(most, top)
            inverse = TOP / most
            code_scale_ref[peer] = most * (1.0 / TOP)
            for k in range(share // 8):
                at = pl.ds(pl.multiple_of(peer * share + k * 8, 8), 8)
                for s in range(segments):
                    lanes = slice(s * LANES, (s + 1) * LANES)
                    code_ref[peer, k * 8 : (k + 1) * 8, lanes] = pack(
                        ends_ref[0, at, lanes], ends_ref[1, at, lanes], inverse
                    )

        for i in range(1, count_x):
            code_peer(to_x(i))
            start(outward, i)
        code_peer(gx)
    else:
        group = 8 // share
        for i in range(rows_y // 8):
            codes, scale = code_rows(i)
            for k in range(group):
                code_scale_ref[i * group + k] = scale
                for s in range(segments):
                    code_ref[i * group + k, :, s * LANES : (s + 1) * LANES] = codes[s][k * share : (k + 1) * share]
        for i in range(1, count_x):
            start(outward, i)
    sides_ref[gx] = code_ref[gx]
    sides_scale_ref[gx] = code_scale_ref[gx]

    if capacity % 8 == 0:
        flatten()
    for s in range(segments):
        lanes = slice(s * LANES, (s + 1) * LANES)
        rhs_ref[...] = jnp.dot(place_ref[s * rows_y : (s + 1) * rows_y], flat_ref[:, : last * LANES], preferred_element_type=F32)

        def solve(i):
            at = pl.ds(pl.multiple_of(i * 8, 8), 8)
            values = []
            for x in range(last):
                side = velocity_ref[x, at, lanes] + rhs_ref[at, x * LANES : (x + 1) * LANES]
                side = side * local_ref[x]
                values.append(side + local_ref[cells_x + x] * values[-1] if x else side)
            value = values[-1]
            inner_ref[last - 1, at, lanes] = value
            for x in range(last - 2, -1, -1):
                value = values[x] + local_ref[cells_x + x] * value
                inner_ref[x, at, lanes] = value

        loop(0, rows_y // 8, solve, unroll=2)

    for i in range(1, count_x):
        finish(outward, i)

    most = jnp.full((share, LANES), 0.0, F32)
    for s in range(segments):
        lanes = slice(s * LANES, (s + 1) * LANES)
        values = []
        after = None
        sides = [unpack(sides_ref[d, :, lanes], sides_scale_ref[d]) for d in range(count_x)]
        for d in range(count_x):
            side = sides[d][0]
            if d + 1 < count_x:
                side = side + couple_ref[3, d : d + 1, :] * sides[d + 1][1]
            if d:
                side = side - couple_ref[2, d : d + 1, :] * values[-1]
            values.append(side * couple_ref[0, d : d + 1, :])
        value = values[-1]
        solved_ref[count_x - 1, :, lanes] = value
        most = jnp.maximum(most, jnp.abs(value))
        for d in range(count_x - 2, -1, -1):
            value = values[d] - couple_ref[1, d : d + 1, :] * value
            solved_ref[d, :, lanes] = value
            most = jnp.maximum(most, jnp.abs(value))

    most = jnp.maximum(jnp.max(most, axis=0, keepdims=True), TINY)
    inverse = TOP / most
    scale = most * (1.0 / TOP)

    def home_code(d):
        home_scale_ref[d] = scale
        before = jnp.where(d > 0, 1.0, 0.0)
        for s in range(segments):
            lanes = slice(s * LANES, (s + 1) * LANES)
            home_ref[d, :, lanes] = pack(
                solved_ref[d, :, lanes], solved_ref[jnp.maximum(d - 1, 0), :, lanes] * before, inverse
            )

    for i in range(1, count_x):
        home_code(to_x(i))
        start(homeward, i)
    home_code(gx)
    back_ref[gx] = home_ref[gx]
    back_scale_ref[gx] = home_scale_ref[gx]
    for i in range(1, devices):
        tile_copy(i, came(i)).wait_send()
    for i in range(1, count_x):
        finish(homeward, i)


def step(viscosity, forces, weights, owner, slots, velocity, grid_x, grid_y, capacity):
    cells_x, cells_y, cells_z = velocity.shape
    blocks, markers, cells = weights.shape
    devices = grid_x * grid_y
    rows = devices * capacity
    share = cells_y // grid_x
    chunks = 2
    dma = pltpu.SemaphoreType.DMA
    vmem = pltpu.VMEM
    anywhere = pl.BlockSpec(memory_space=pl.ANY)
    whole = pl.BlockSpec(memory_space=pltpu.VMEM)
    line = (grid_x, share, cells_z)
    line_scale = (grid_x, 1, LANES)

    def keep(value):
        return pltpu.with_memory_space_constraint(value, pltpu.HBM)

    return pl.pallas_call(
        functools.partial(step_kernel, grid_x, grid_y, capacity, chunks),
        out_shape=(
            jax.ShapeDtypeStruct((cells_x - 1, cells_y, cells_z), F32),
            jax.ShapeDtypeStruct(line, jnp.int32),
            jax.ShapeDtypeStruct(line_scale, F32),
            jax.ShapeDtypeStruct((2 * (cells_x - 1), 8, LANES), F32),
        ),
        in_specs=[anywhere] * 6,
        out_specs=(whole,) * 4,
        scratch_shapes=[
            pltpu.SMEM((cells_x,), F32),
            vmem((markers, blocks), BF16),
            vmem((1, blocks), jnp.int32),
            vmem((1, blocks), jnp.int32),
            vmem((chunks, blocks, markers, cells // chunks), BF16),
            vmem((cells_x, cells_y, cells_z), F32),
            vmem((rows, blocks * markers), BF16),
            vmem((devices, capacity, cells), BF16),
            vmem((devices, capacity, cells), BF16),
            vmem((devices, 1, LANES), F32),
            vmem((devices, 1, LANES), F32),
            vmem((cells_z // LANES * cells_y, rows), BF16),
            vmem((rows, 2 * LANES), F32),
            vmem((2, cells_y, cells_z), F32),
            vmem((2 * cells_x, 8, LANES), F32),
            vmem((2 * cells_x, 8, LANES), F32),
            vmem((4, grid_x, LANES), F32),
            vmem(line, jnp.int32),
            vmem(line_scale, F32),
            vmem(line, jnp.int32),
            vmem(line_scale, F32),
            vmem(line, F32),
            vmem(line, jnp.int32),
            vmem(line_scale, F32),
            vmem((cells_y, (cells_x - 1) * LANES), F32),
            vmem((rows, cells), BF16),
            dma((5,)),
            dma((chunks,)),
            dma((devices,)),
            dma((devices,)),
            dma((devices,)),
            dma((devices,)),
        ]
        + [dma((grid_x,))] * 8,
        compiler_params=pltpu.CompilerParams(
            collective_id=0, has_side_effects=True, vmem_limit_bytes=40 << 20
        ),
    )(
        keep(viscosity), keep(forces), keep(weights), keep(owner), keep(slots), keep(velocity)
    )


def rows_of(ref, i):
    rows = ref.shape[1]
    if rows % 8 == 0:
        start = pl.multiple_of(lax.rem(i * 8, rows), 8)
        return lambda lane: ref[i * 8 // rows, pl.ds(start, 8), lane]
    share = 8 // rows
    return lambda lane: jnp.concatenate([ref[i * share + k, :, lane] for k in range(share)], axis=0)


def scale_of(ref, i, rows):
    if rows % 8 == 0:
        return ref[i * 8 // rows]
    share = 8 // rows
    parts = [jnp.broadcast_to(ref[i * share + k], (rows, LANES)) for k in range(share)]
    return jnp.concatenate(parts, axis=0)


def final_kernel(parts, inner_ref, back_ref, scale_ref, mix_ref, out_hbm, out_ref, sem):
    count, rows_y, cells_z = inner_ref.shape
    rows = rows_y // parts

    def copy(p):
        at = pl.ds(pl.multiple_of(p * rows, 8), rows)
        return pltpu.make_async_copy(out_ref.at[:, at, :], out_hbm.at[:, at, :], sem.at[p])

    def chunk(i):
        at = pl.ds(pl.multiple_of(i * 8, 8), 8)
        codes = rows_of(back_ref, i)
        scale = scale_of(scale_ref, i, back_ref.shape[1])
        for c in range(cells_z // LANES):
            lane = slice(c * LANES, (c + 1) * LANES)
            last, before = unpack(codes(lane), scale)
            for x in range(count):
                out_ref[x, at, lane] = (
                    inner_ref[x, at, lane] + mix_ref[x] * before + mix_ref[count + x] * last
                )
            out_ref[count, at, lane] = last

    def part(p, carry):
        for k in range(rows // 8):
            chunk(p * (rows // 8) + k)
        copy(p).start()
        return carry

    def done(p, carry):
        copy(p).wait()
        return carry

    lax.fori_loop(0, parts, part, 0)
    lax.fori_loop(0, parts, done, 0)


def final(inner, back, scale, mix):
    count, cells_y, cells_z = inner.shape
    parts = 8
    shape = (count + 1, cells_y, cells_z)
    return pl.pallas_call(
        functools.partial(final_kernel, parts),
        out_shape=jax.ShapeDtypeStruct(shape, F32),
        in_specs=[pl.BlockSpec(memory_space=pltpu.VMEM)] * 4,
        out_specs=pl.BlockSpec(memory_space=pl.ANY),
        scratch_shapes=[pltpu.VMEM(shape, F32), pltpu.SemaphoreType.DMA((parts,))],
        compiler_params=pltpu.CompilerParams(vmem_limit_bytes=24 << 20),
    )(inner, back, scale, mix)


def per_device(velocity, viscosity, marker_forces, spread_weights, block_owner, tile_slot):
    grid_x, grid_y = lax.axis_size("gx"), lax.axis_size("gy")
    blocks = spread_weights.shape[0]
    capacity = max(2, 2 * blocks // (grid_x * grid_y))
    inner, back, scale, mix = step(
        viscosity,
        marker_forces.T,
        spread_weights,
        block_owner.reshape(1, blocks),
        tile_slot.reshape(1, blocks),
        velocity,
        grid_x,
        grid_y,
        capacity,
    )
    return final(inner, back, scale, mix)


def solution(mesh):
    placed = (
        P("gx", "gy", None),
        P("gx"),
        P(("gx", "gy"), None),
        P(("gx", "gy"), None, None),
        P(("gx", "gy"), None),
        P(("gx", "gy")),
    )
    return jax.shard_map(
        per_device, mesh=mesh, in_specs=placed, out_specs=P("gx", "gy", None), check_vma=False
    )
```

```python
import functools

import jax
import jax.numpy as jnp
from jax import lax
from jax.experimental import pallas as pl
from jax.experimental.pallas import tpu as pltpu
from jax.sharding import PartitionSpec as P

F32 = jnp.float32
BF16 = jnp.bfloat16
BASE = 256
LANES = 128
VISC_LANE = 64
TOP = 32767.0
TINY = 1e-30


def iota(shape, axis):
    return lax.broadcasted_iota(jnp.int32, shape, axis)


def nt_dot(a, b):
    return lax.dot_general(a, b, (((1,), (1,)), ((), ())), preferred_element_type=F32)


def tn_dot(a, b):
    return lax.dot_general(a, b, (((0,), (0,)), ((), ())), preferred_element_type=F32)


def factor(visc):
    inverse, ratio = [], []
    for x in range(len(visc) - 1):
        pivot = 1.0 + 2.0 * visc[x]
        if x:
            pivot = pivot - visc[x] * ratio[-1]
        inverse.append(1.0 / pivot)
        ratio.append(visc[x] * inverse[-1])
    return inverse, ratio


def spikes(inverse, ratio):
    count = len(inverse)
    left = [inverse[0]]
    for x in range(1, count):
        left.append(ratio[x] * left[-1])
    for x in range(count - 2, -1, -1):
        left[x] = left[x] + ratio[x] * left[x + 1]
    right = [inverse[-1]]
    for x in range(count - 2, -1, -1):
        right.append(ratio[x] * right[-1])
    return left, right[::-1]


def end_weights(visc, inverse, ratio):
    count = len(inverse)
    last, run = [], visc[-1]
    for x in range(count - 1, -1, -1):
        last.append(run * inverse[x])
        run = run * ratio[x]
    reach = [jnp.ones_like(inverse[0])]
    for x in range(count - 1):
        reach.append(reach[-1] * ratio[x])
    first, total = [], None
    for x in range(count - 1, -1, -1):
        total = reach[x] if total is None else reach[x] + ratio[x + 1] * total
        first.append(visc[0] * inverse[x] * total)
    return last[::-1], first[::-1]


def couple(visc, stride, out_ref):
    rows, lanes = visc[0].shape
    count = rows // stride
    inverse, ratio = factor(visc)
    left, right = spikes(inverse, ratio)
    row = iota((rows, lanes), 0)

    def following(value):
        moved = jnp.concatenate([value[stride:], value[:stride]], axis=0)
        return jnp.where(row >= rows - stride, 0.0, moved)

    sep, inner, first = visc[-1], visc[-2], visc[0]
    lower = jnp.where(row >= stride, -sep * first * left[-1], 0.0)
    center = 1.0 + 2.0 * sep - sep * inner * right[-1] - sep * following(first * left[0])
    upper = -sep * following(inner * right[0])
    final_rows = row >= rows - stride
    held = jnp.where(final_rows, 0.0, sep / jnp.where(final_rows, 1.0, following(first)))
    previous = jnp.zeros((1, lanes), F32)
    for d in range(count):
        at = slice(d * stride, d * stride + 1)
        pivot = center[at] - lower[at] * previous
        inv = 1.0 / pivot
        previous = upper[at] * inv
        out_ref[0, d : d + 1, :] = inv
        out_ref[1, d : d + 1, :] = previous
        out_ref[2, d : d + 1, :] = lower[at]
        out_ref[3, d : d + 1, :] = held[at]


def peers(me, count):
    if count & (count - 1):
        return (lambda k: lax.rem(me + k, count)), (lambda k: lax.rem(me + count - k, count))
    steps, bit = [], 1
    while bit < count:
        steps.append(bit - 2 * bit * lax.rem(me // bit, 2))
        bit *= 2

    def peer(k):
        moved = me
        for n, step in enumerate(steps):
            if k >> n & 1:
                moved = moved + step
        return moved

    return peer, peer


def peak(values):
    most = jnp.abs(values[0])
    for value in values[1:]:
        most = jnp.maximum(most, jnp.abs(value))
    return jnp.maximum(jnp.max(most, axis=0, keepdims=True), TINY)


def pack(high, low, inverse):
    high = jnp.round(high * inverse).astype(jnp.int32)
    low = jnp.round(low * inverse).astype(jnp.int32)
    return high * 65536 + low


def unpack(code, scale):
    low = (code << 16) >> 16
    high = (code - low) >> 16
    return high.astype(F32) * scale, low.astype(F32) * scale


def step_kernel(
    count_x, count_y, capacity, chunks,
    visc_hbm, forces_hbm, weights_hbm, owner_hbm, slot_hbm, velocity_hbm,
    inner_ref, back_ref, back_scale_ref, mix_ref,
    visc_ref, forces_ref, owner_ref, slot_ref, weights_ref, velocity_ref,
    spread_ref, outgoing_ref, tiles_ref, meta_ref, metas_ref, place_ref, tile_ends_ref, ends_ref,
    local_ref, weight_ref, couple_ref, code_ref, code_scale_ref, sides_ref, sides_scale_ref,
    solved_ref, home_ref, home_scale_ref, rhs_ref, flat_ref,
    own, wsem, tile_send, tile_recv, meta_sem, line_sem,
):
    devices = count_x * count_y
    cells_x, rows_y, cells_z = velocity_ref.shape
    markers, blocks = forces_ref.shape
    width = outgoing_ref.shape[3]
    cells = chunks * width
    wide = blocks * markers
    rows = devices * capacity
    share = code_ref.shape[1]
    segments = cells_z // LANES
    last = cells_x - 1
    gx, gy = lax.axis_index("gx"), lax.axis_index("gy")
    me = gx * count_y + gy

    to_x, from_x = peers(gx, count_x)
    to_y, from_y = peers(gy, count_y)

    def device(i):
        return (to_x(i // count_y), to_y(i % count_y))

    def index(i):
        px, py = device(i)
        return px * count_y + py

    def came(i):
        return from_x(i // count_y) * count_y + from_y(i % count_y)

    def loop(first, end, body, unroll=1):
        def step(i, carry):
            body(i)
            return carry

        lax.fori_loop(first, end, step, 0, unroll=unroll)

    barrier = pltpu.get_barrier_semaphore()

    for i in range(1, devices):
        pl.semaphore_signal(
            barrier, inc=1, device_id=device(i), device_id_type=pl.DeviceIdType.MESH
        )

    small = [
        pltpu.make_async_copy(source, target, own.at[k])
        for k, (source, target) in enumerate(
            ((owner_hbm, owner_ref), (forces_hbm, forces_ref), (slot_hbm, slot_ref), (visc_hbm, visc_ref))
        )
    ]
    for copy in small:
        copy.start()

    def weight_copy(c):
        at = pl.ds(pl.multiple_of(c * width, width), width)
        return pltpu.make_async_copy(weights_hbm.at[:, :, at], weights_ref.at[c], wsem.at[c])

    loop(0, chunks, lambda c: weight_copy(c).start())
    velocity_copy = pltpu.make_async_copy(velocity_hbm, velocity_ref, own.at[4])
    for copy in small:
        copy.wait()

    owner = owner_ref[...]
    matches = (iota((devices, blocks), 0) == owner).astype(BF16)
    earlier = (iota((blocks, blocks), 0) < iota((blocks, blocks), 1)).astype(BF16)
    counts = jnp.dot(matches, earlier, preferred_element_type=F32)
    rank = jnp.sum(counts * matches.astype(F32), axis=0, keepdims=True).astype(jnp.int32)
    target = owner * capacity + rank
    select = (iota((rows, blocks), 0) == target).astype(BF16)
    choose = (iota((markers, wide), 1) % markers == iota((markers, wide), 0)).astype(BF16)
    tiled = tn_dot(forces_ref[...], choose)
    offset = iota((blocks, wide), 1) - iota((blocks, wide), 0) * markers
    spread = jnp.where((offset >= 0) & (offset < markers), tiled, 0.0).astype(BF16)
    spread_ref[...] = jnp.dot(select, spread, preferred_element_type=F32).astype(BF16)

    number = slot_ref[...] + 1
    high = number // BASE
    ranked = iota((LANES, blocks), 0) == rank
    digits = [jnp.where(ranked, d, 0).astype(F32).astype(BF16) for d in (high, number - high * BASE)]
    meta = nt_dot(matches, digits[0]) * BASE + nt_dot(matches, digits[1])
    lane = iota((1, LANES), 1)
    viscous = jnp.zeros((1, LANES), F32)
    for x in range(cells_x):
        viscous = jnp.where(lane == VISC_LANE + x, visc_ref[x], viscous)
    meta = meta + viscous
    for d in range(devices):
        meta_ref[d] = meta[d : d + 1]

    def remote(source, target, send, receive, peer):
        return pltpu.make_async_remote_copy(
            src_ref=source,
            dst_ref=target,
            send_sem=send,
            recv_sem=receive,
            device_id=peer,
            device_id_type=pl.DeviceIdType.MESH,
        )

    def several(source, target, send, receive, number):
        at = pl.ds(0, number)
        return remote(source.at[at], target.at[at], send, receive, device(1))

    span = max(1, devices // 4)

    def tile_copy(c, i):
        return remote(
            outgoing_ref.at[index(i), c], tiles_ref.at[me, c],
            tile_send.at[0], tile_recv.at[i // span], device(i),
        )

    def tiles_come(group):
        number = span if group else span - 1
        several(outgoing_ref, tiles_ref, tile_send.at[0], tile_recv.at[group], number).wait_recv()

    def meta_copy(i):
        return remote(
            meta_ref.at[index(i)], metas_ref.at[me], meta_sem.at[0], meta_sem.at[1], device(i)
        )

    for c in range(chunks):
        weight_copy(c).wait()
        out = jnp.dot(
            spread_ref[...], weights_ref[c].reshape(wide, width), preferred_element_type=F32
        )
        if capacity % 8 == 0:
            outgoing_ref[:, c] = out.reshape(devices, capacity, width).astype(BF16)
        else:
            for d in range(devices):
                outgoing_ref[d, c] = out[d * capacity : (d + 1) * capacity].astype(BF16)
        if c == 0:
            pl.semaphore_wait(barrier, devices - 1)
            for i in range(1, devices):
                meta_copy(i).start()
        for i in range(1, devices):
            tile_copy(c, i).start()
        tiles_ref[me, c] = outgoing_ref[me, c]
    velocity_copy.start()
    metas_ref[me] = meta_ref[me]

    visc = [jnp.full((8, LANES), visc_ref[x], F32) for x in range(cells_x)]
    inverse, ratio = factor(visc)
    for x in range(last):
        local_ref[x] = inverse[x]
        local_ref[cells_x + x] = ratio[x]
    to_last, to_first = end_weights(visc, inverse, ratio)
    for x in range(last):
        weight_ref[x] = to_last[x]
        weight_ref[cells_x + x] = to_first[x]
    left, right = spikes(inverse, ratio)
    for x in range(last):
        mix_ref[x] = visc[0] * left[x]
        mix_ref[last + x] = visc[last - 1] * right[x]

    def ends_of(side):
        value = side(0)
        high, low = value * weight_ref[0], value * weight_ref[cells_x]
        for x in range(1, last):
            value = side(x)
            high = high + value * weight_ref[x]
            low = low + value * weight_ref[cells_x + x]
        return high + side(last), low

    velocity_copy.wait()

    def velocity_ends(i):
        at = pl.ds(pl.multiple_of(i * 8, 8), 8)
        for s in range(segments):
            lanes = slice(s * LANES, (s + 1) * LANES)
            high, low = ends_of(lambda x: velocity_ref[x, at, lanes])
            ends_ref[0, at, lanes] = high
            ends_ref[1, at, lanes] = low

    loop(0, rows_y // 8, velocity_ends)

    several(meta_ref, metas_ref, meta_sem.at[0], meta_sem.at[1], devices - 1).wait()
    metas = jnp.concatenate([metas_ref[d] for d in range(devices)], axis=0)
    couple(
        [
            jnp.broadcast_to(metas[:, VISC_LANE + x : VISC_LANE + x + 1], (devices, LANES))
            for x in range(cells_x)
        ],
        count_y,
        couple_ref,
    )
    lane = iota((devices, LANES), 1)
    numbers = jnp.where(lane < capacity, metas, 0.0).astype(jnp.int32)
    high = numbers // BASE
    expand = (iota((LANES, rows), 1) % capacity == iota((LANES, rows), 0)).astype(BF16)
    number = jnp.zeros((devices, rows), F32)
    for digit, base in ((high, float(BASE)), (numbers - high * BASE, 1.0)):
        number = number + base * jnp.dot(
            digit.astype(F32).astype(BF16), expand, preferred_element_type=F32
        )
    offset = iota((devices, rows), 1) - iota((devices, rows), 0) * capacity
    number = jnp.where((offset >= 0) & (offset < capacity), number, 0.0)
    number = jnp.sum(number, axis=0, keepdims=True).astype(jnp.int32) - 1
    for s in range(segments):
        place_ref[s * rows_y : (s + 1) * rows_y] = (
            iota((rows_y, rows), 0) * segments + s == number
        ).astype(BF16)

    def tile_cells(slot, x):
        c, lane = divmod(x * LANES, width)
        return tiles_ref[slot, c, :, lane : lane + LANES].astype(F32)

    def tile_ends(slot):
        at = pl.ds(pl.multiple_of(slot * capacity, capacity), capacity)
        high, low = ends_of(lambda x: tile_cells(slot, x))
        tile_ends_ref[at, :LANES] = high
        tile_ends_ref[at, LANES:] = low

    def flatten():
        for c in range(chunks):
            at = slice(c * width, (c + 1) * width)
            if capacity % 8 == 0:
                flat_ref[:, at] = tiles_ref[:, c].astype(F32).reshape(rows, width).astype(BF16)
            else:
                parts = [tiles_ref[d, c].astype(F32) for d in range(devices)]
                flat_ref[:, at] = jnp.concatenate(parts, axis=0).astype(BF16)

    if capacity % 8 == 0:
        tile_ends(me)

        for group in range(devices // span):
            if group or span > 1:
                tiles_come(group)
            for i in range(max(1, group * span), (group + 1) * span):
                tile_ends(came(i))
    else:
        for group in range(devices // span):
            if group or span > 1:
                tiles_come(group)
        flatten()

        def flat_ends(i):
            at = pl.ds(pl.multiple_of(i * 8, 8), 8)
            high, low = ends_of(lambda x: flat_ref[at, x * LANES : (x + 1) * LANES].astype(F32))
            tile_ends_ref[at, :LANES] = high
            tile_ends_ref[at, LANES:] = low

        loop(0, rows // 8, flat_ends)

    found = tile_ends_ref[...]
    coarse = found.astype(BF16)
    fine = (found - coarse.astype(F32)).astype(BF16)
    both = jnp.concatenate([coarse, fine], axis=1)
    placed = jnp.dot(place_ref[...], both, preferred_element_type=F32)
    for s in range(segments):
        lanes = slice(s * LANES, (s + 1) * LANES)
        part = placed[s * rows_y : (s + 1) * rows_y]
        for w in (0, 1):
            ends_ref[w, :, lanes] = ends_ref[w, :, lanes] + (
                part[:, w * LANES : (w + 1) * LANES] + part[:, (w + 2) * LANES : (w + 3) * LANES]
            )

    outward = ((code_ref, sides_ref, 0), (code_scale_ref, sides_scale_ref, 2))
    homeward = ((home_ref, back_ref, 4), (home_scale_ref, back_scale_ref, 6))

    def start(groups, i):
        peer = to_x(i)
        for source, target, k in groups:
            remote(
                source.at[peer], target.at[gx], line_sem.at[k], line_sem.at[k + 1], (peer, gy)
            ).start()

    def finish(groups):
        for source, target, k in groups:
            several(source, target, line_sem.at[k], line_sem.at[k + 1], count_x - 1).wait()

    def code_rows(i):
        at = pl.ds(pl.multiple_of(i * 8, 8), 8)
        pairs = []
        for s in range(segments):
            lanes = slice(s * LANES, (s + 1) * LANES)
            pairs.append((ends_ref[0, at, lanes], ends_ref[1, at, lanes]))
        most = peak([value for pair in pairs for value in pair])
        inverse = TOP / most
        codes = [pack(high, low, inverse) for high, low in pairs]
        scale = most * (1.0 / TOP)
        return codes, scale

    if share % 8 == 0:

        def code_peer(peer):
            most = None
            for k in range(share // 8):
                at = pl.ds(pl.multiple_of(peer * share + k * 8, 8), 8)
                top = peak([ends_ref[w, at, s * LANES : (s + 1) * LANES] for s in range(segments) for w in (0, 1)])
                most = top if most is None else jnp.maximum(most, top)
            inverse = TOP / most
            code_scale_ref[peer] = most * (1.0 / TOP)
            for k in range(share // 8):
                at = pl.ds(pl.multiple_of(peer * share + k * 8, 8), 8)
                for s in range(segments):
                    lanes = slice(s * LANES, (s + 1) * LANES)
                    code_ref[peer, k * 8 : (k + 1) * 8, lanes] = pack(
                        ends_ref[0, at, lanes], ends_ref[1, at, lanes], inverse
                    )

        for i in range(1, count_x):
            code_peer(to_x(i))
            start(outward, i)
        code_peer(gx)
    else:
        group = 8 // share
        for i in range(rows_y // 8):
            codes, scale = code_rows(i)
            for k in range(group):
                code_scale_ref[i * group + k] = scale
                for s in range(segments):
                    code_ref[i * group + k, :, s * LANES : (s + 1) * LANES] = codes[s][k * share : (k + 1) * share]
        for i in range(1, count_x):
            start(outward, i)
    sides_ref[gx] = code_ref[gx]
    sides_scale_ref[gx] = code_scale_ref[gx]

    if capacity % 8 == 0:
        flatten()
    for s in range(segments):
        lanes = slice(s * LANES, (s + 1) * LANES)
        rhs_ref[...] = jnp.dot(place_ref[s * rows_y : (s + 1) * rows_y], flat_ref[:, : last * LANES], preferred_element_type=F32)

        def solve(i):
            at = pl.ds(pl.multiple_of(i * 8, 8), 8)
            values = []
            for x in range(last):
                side = velocity_ref[x, at, lanes] + rhs_ref[at, x * LANES : (x + 1) * LANES]
                side = side * local_ref[x]
                values.append(side + local_ref[cells_x + x] * values[-1] if x else side)
            value = values[-1]
            inner_ref[last - 1, at, lanes] = value
            for x in range(last - 2, -1, -1):
                value = values[x] + local_ref[cells_x + x] * value
                inner_ref[x, at, lanes] = value

        loop(0, rows_y // 8, solve, unroll=2)

    finish(outward)

    most = jnp.full((share, LANES), 0.0, F32)
    for s in range(segments):
        lanes = slice(s * LANES, (s + 1) * LANES)
        values = []
        after = None
        sides = [unpack(sides_ref[d, :, lanes], sides_scale_ref[d]) for d in range(count_x)]
        for d in range(count_x):
            side = sides[d][0]
            if d + 1 < count_x:
                side = side + couple_ref[3, d : d + 1, :] * sides[d + 1][1]
            if d:
                side = side - couple_ref[2, d : d + 1, :] * values[-1]
            values.append(side * couple_ref[0, d : d + 1, :])
        value = values[-1]
        solved_ref[count_x - 1, :, lanes] = value
        most = jnp.maximum(most, jnp.abs(value))
        for d in range(count_x - 2, -1, -1):
            value = values[d] - couple_ref[1, d : d + 1, :] * value
            solved_ref[d, :, lanes] = value
            most = jnp.maximum(most, jnp.abs(value))

    most = jnp.maximum(jnp.max(most, axis=0, keepdims=True), TINY)
    inverse = TOP / most
    scale = most * (1.0 / TOP)

    def home_code(d):
        home_scale_ref[d] = scale
        before = jnp.where(d > 0, 1.0, 0.0)
        for s in range(segments):
            lanes = slice(s * LANES, (s + 1) * LANES)
            home_ref[d, :, lanes] = pack(
                solved_ref[d, :, lanes], solved_ref[jnp.maximum(d - 1, 0), :, lanes] * before, inverse
            )

    for i in range(1, count_x):
        home_code(to_x(i))
        start(homeward, i)
    home_code(gx)
    back_ref[gx] = home_ref[gx]
    back_scale_ref[gx] = home_scale_ref[gx]
    several(outgoing_ref, tiles_ref, tile_send.at[0], tile_recv.at[0], devices - 1).wait_send()
    finish(homeward)


def step(viscosity, forces, weights, owner, slots, velocity, grid_x, grid_y, capacity):
    cells_x, cells_y, cells_z = velocity.shape
    blocks, markers, cells = weights.shape
    devices = grid_x * grid_y
    rows = devices * capacity
    share = cells_y // grid_x
    chunks = 4
    dma = pltpu.SemaphoreType.DMA
    vmem = pltpu.VMEM
    anywhere = pl.BlockSpec(memory_space=pl.ANY)
    whole = pl.BlockSpec(memory_space=pltpu.VMEM)
    line = (grid_x, share, cells_z)
    line_scale = (grid_x, 1, LANES)

    def keep(value):
        return pltpu.with_memory_space_constraint(value, pltpu.HBM)

    return pl.pallas_call(
        functools.partial(step_kernel, grid_x, grid_y, capacity, chunks),
        out_shape=(
            jax.ShapeDtypeStruct((cells_x - 1, cells_y, cells_z), F32),
            jax.ShapeDtypeStruct(line, jnp.int32),
            jax.ShapeDtypeStruct(line_scale, F32),
            jax.ShapeDtypeStruct((2 * (cells_x - 1), 8, LANES), F32),
        ),
        in_specs=[anywhere] * 6,
        out_specs=(whole,) * 4,
        scratch_shapes=[
            pltpu.SMEM((cells_x,), F32),
            vmem((markers, blocks), BF16),
            vmem((1, blocks), jnp.int32),
            vmem((1, blocks), jnp.int32),
            vmem((chunks, blocks, markers, cells // chunks), BF16),
            vmem((cells_x, cells_y, cells_z), F32),
            vmem((rows, blocks * markers), BF16),
            vmem((devices, chunks, capacity, cells // chunks), BF16),
            vmem((devices, chunks, capacity, cells // chunks), BF16),
            vmem((devices, 1, LANES), F32),
            vmem((devices, 1, LANES), F32),
            vmem((cells_z // LANES * cells_y, rows), BF16),
            vmem((rows, 2 * LANES), F32),
            vmem((2, cells_y, cells_z), F32),
            vmem((2 * cells_x, 8, LANES), F32),
            vmem((2 * cells_x, 8, LANES), F32),
            vmem((4, grid_x, LANES), F32),
            vmem(line, jnp.int32),
            vmem(line_scale, F32),
            vmem(line, jnp.int32),
            vmem(line_scale, F32),
            vmem(line, F32),
            vmem(line, jnp.int32),
            vmem(line_scale, F32),
            vmem((cells_y, (cells_x - 1) * LANES), F32),
            vmem((rows, cells), BF16),
            dma((5,)),
            dma((chunks,)),
            dma((1,)),
            dma((4,)),
            dma((2,)),
            dma((8,)),
        ],
        compiler_params=pltpu.CompilerParams(
            collective_id=0, has_side_effects=True, vmem_limit_bytes=40 << 20
        ),
    )(
        keep(viscosity), keep(forces), keep(weights), keep(owner), keep(slots), keep(velocity)
    )


def rows_of(ref, i):
    rows = ref.shape[1]
    if rows % 8 == 0:
        start = pl.multiple_of(lax.rem(i * 8, rows), 8)
        return lambda lane: ref[i * 8 // rows, pl.ds(start, 8), lane]
    share = 8 // rows
    return lambda lane: jnp.concatenate([ref[i * share + k, :, lane] for k in range(share)], axis=0)


def scale_of(ref, i, rows):
    if rows % 8 == 0:
        return ref[i * 8 // rows]
    share = 8 // rows
    parts = [jnp.broadcast_to(ref[i * share + k], (rows, LANES)) for k in range(share)]
    return jnp.concatenate(parts, axis=0)


def final_kernel(parts, inner_ref, back_ref, scale_ref, mix_ref, out_hbm, out_ref, sem):
    count, rows_y, cells_z = inner_ref.shape
    rows = rows_y // parts

    def copy(p):
        at = pl.ds(pl.multiple_of(p * rows, 8), rows)
        return pltpu.make_async_copy(out_ref.at[:, at, :], out_hbm.at[:, at, :], sem.at[p])

    def chunk(i):
        at = pl.ds(pl.multiple_of(i * 8, 8), 8)
        codes = rows_of(back_ref, i)
        scale = scale_of(scale_ref, i, back_ref.shape[1])
        for c in range(cells_z // LANES):
            lane = slice(c * LANES, (c + 1) * LANES)
            last, before = unpack(codes(lane), scale)
            for x in range(count):
                out_ref[x, at, lane] = (
                    inner_ref[x, at, lane] + mix_ref[x] * before + mix_ref[count + x] * last
                )
            out_ref[count, at, lane] = last

    def part(p, carry):
        for k in range(rows // 8):
            chunk(p * (rows // 8) + k)
        copy(p).start()
        return carry

    def done(p, carry):
        copy(p).wait()
        return carry

    lax.fori_loop(0, parts, part, 0)
    lax.fori_loop(0, parts, done, 0)


def final(inner, back, scale, mix):
    count, cells_y, cells_z = inner.shape
    parts = 8
    shape = (count + 1, cells_y, cells_z)
    return pl.pallas_call(
        functools.partial(final_kernel, parts),
        out_shape=jax.ShapeDtypeStruct(shape, F32),
        in_specs=[pl.BlockSpec(memory_space=pltpu.VMEM)] * 4,
        out_specs=pl.BlockSpec(memory_space=pl.ANY),
        scratch_shapes=[pltpu.VMEM(shape, F32), pltpu.SemaphoreType.DMA((parts,))],
        compiler_params=pltpu.CompilerParams(vmem_limit_bytes=24 << 20),
    )(inner, back, scale, mix)


def per_device(velocity, viscosity, marker_forces, spread_weights, block_owner, tile_slot):
    grid_x, grid_y = lax.axis_size("gx"), lax.axis_size("gy")
    blocks = spread_weights.shape[0]
    capacity = max(2, 2 * blocks // (grid_x * grid_y))
    inner, back, scale, mix = step(
        viscosity,
        marker_forces.T,
        spread_weights,
        block_owner.reshape(1, blocks),
        tile_slot.reshape(1, blocks),
        velocity,
        grid_x,
        grid_y,
        capacity,
    )
    return final(inner, back, scale, mix)


def solution(mesh):
    placed = (
        P("gx", "gy", None),
        P("gx"),
        P(("gx", "gy"), None),
        P(("gx", "gy"), None, None),
        P(("gx", "gy"), None),
        P(("gx", "gy")),
    )
    return jax.shard_map(
        per_device, mesh=mesh, in_specs=placed, out_specs=P("gx", "gy", None), check_vma=False
    )
```

```python
import functools

import jax
import jax.numpy as jnp
from jax import lax
from jax.experimental import pallas as pl
from jax.experimental.pallas import tpu as pltpu
from jax.sharding import PartitionSpec as P

F32 = jnp.float32
BF16 = jnp.bfloat16
BASE = 256
LANES = 128
VISC_LANE = 64
TOP = 32767.0
TINY = 1e-30


def iota(shape, axis):
    return lax.broadcasted_iota(jnp.int32, shape, axis)


def nt_dot(a, b):
    return lax.dot_general(a, b, (((1,), (1,)), ((), ())), preferred_element_type=F32)


def tn_dot(a, b):
    return lax.dot_general(a, b, (((0,), (0,)), ((), ())), preferred_element_type=F32)


def factor(visc):
    inverse, ratio = [], []
    for x in range(len(visc) - 1):
        pivot = 1.0 + 2.0 * visc[x]
        if x:
            pivot = pivot - visc[x] * ratio[-1]
        inverse.append(1.0 / pivot)
        ratio.append(visc[x] * inverse[-1])
    return inverse, ratio


def spikes(inverse, ratio):
    count = len(inverse)
    left = [inverse[0]]
    for x in range(1, count):
        left.append(ratio[x] * left[-1])
    for x in range(count - 2, -1, -1):
        left[x] = left[x] + ratio[x] * left[x + 1]
    right = [inverse[-1]]
    for x in range(count - 2, -1, -1):
        right.append(ratio[x] * right[-1])
    return left, right[::-1]


def end_weights(visc, inverse, ratio):
    count = len(inverse)
    last, run = [], visc[-1]
    for x in range(count - 1, -1, -1):
        last.append(run * inverse[x])
        run = run * ratio[x]
    reach = [jnp.ones_like(inverse[0])]
    for x in range(count - 1):
        reach.append(reach[-1] * ratio[x])
    first, total = [], None
    for x in range(count - 1, -1, -1):
        total = reach[x] if total is None else reach[x] + ratio[x + 1] * total
        first.append(visc[0] * inverse[x] * total)
    return last[::-1], first[::-1]


def couple(visc, stride, out_ref):
    rows, lanes = visc[0].shape
    count = rows // stride
    inverse, ratio = factor(visc)
    left, right = spikes(inverse, ratio)
    row = iota((rows, lanes), 0)

    def following(value):
        moved = jnp.concatenate([value[stride:], value[:stride]], axis=0)
        return jnp.where(row >= rows - stride, 0.0, moved)

    sep, inner, first = visc[-1], visc[-2], visc[0]
    lower = jnp.where(row >= stride, -sep * first * left[-1], 0.0)
    center = 1.0 + 2.0 * sep - sep * inner * right[-1] - sep * following(first * left[0])
    upper = -sep * following(inner * right[0])
    final_rows = row >= rows - stride
    held = jnp.where(final_rows, 0.0, sep / jnp.where(final_rows, 1.0, following(first)))
    previous = jnp.zeros((1, lanes), F32)
    for d in range(count):
        at = slice(d * stride, d * stride + 1)
        pivot = center[at] - lower[at] * previous
        inv = 1.0 / pivot
        previous = upper[at] * inv
        out_ref[0, d : d + 1, :] = inv
        out_ref[1, d : d + 1, :] = previous
        out_ref[2, d : d + 1, :] = lower[at]
        out_ref[3, d : d + 1, :] = held[at]


def peers(me, count):
    if count & (count - 1):
        return (lambda k: lax.rem(me + k, count)), (lambda k: lax.rem(me + count - k, count))
    steps, bit = [], 1
    while bit < count:
        steps.append(bit - 2 * bit * lax.rem(me // bit, 2))
        bit *= 2

    def peer(k):
        moved = me
        for n, step in enumerate(steps):
            if k >> n & 1:
                moved = moved + step
        return moved

    return peer, peer


def peak(values):
    most = jnp.abs(values[0])
    for value in values[1:]:
        most = jnp.maximum(most, jnp.abs(value))
    return jnp.maximum(jnp.max(most, axis=0, keepdims=True), TINY)


def pack(high, low, inverse):
    high = jnp.round(high * inverse).astype(jnp.int32)
    low = jnp.round(low * inverse).astype(jnp.int32)
    return high * 65536 + low


def unpack(code, scale):
    low = (code << 16) >> 16
    high = (code - low) >> 16
    return high.astype(F32) * scale, low.astype(F32) * scale


def step_kernel(
    count_x, count_y, capacity, chunks,
    visc_hbm, forces_hbm, weights_hbm, owner_hbm, slot_hbm, velocity_hbm,
    inner_ref, back_ref, back_scale_ref, mix_ref,
    visc_ref, forces_ref, owner_ref, slot_ref, weights_ref, velocity_ref,
    spread_ref, outgoing_ref, tiles_ref, meta_ref, metas_ref, place_ref, tile_ends_ref, ends_ref,
    local_ref, weight_ref, couple_ref, code_ref, code_scale_ref, sides_ref, sides_scale_ref,
    solved_ref, home_ref, home_scale_ref, rhs_ref, flat_ref,
    own, wsem, tile_send, tile_recv, meta_sem, line_sem,
):
    devices = count_x * count_y
    cells_x, rows_y, cells_z = velocity_ref.shape
    markers, blocks = forces_ref.shape
    width = outgoing_ref.shape[3]
    cells = chunks * width
    wide = blocks * markers
    rows = devices * capacity
    share = code_ref.shape[1]
    segments = cells_z // LANES
    last = cells_x - 1
    gx, gy = lax.axis_index("gx"), lax.axis_index("gy")
    me = gx * count_y + gy

    to_x, from_x = peers(gx, count_x)
    to_y, from_y = peers(gy, count_y)

    def device(i):
        return (to_x(i // count_y), to_y(i % count_y))

    def index(i):
        px, py = device(i)
        return px * count_y + py

    def came(i):
        return from_x(i // count_y) * count_y + from_y(i % count_y)

    def loop(first, end, body, unroll=1):
        def step(i, carry):
            body(i)
            return carry

        lax.fori_loop(first, end, step, 0, unroll=unroll)

    barrier = pltpu.get_barrier_semaphore()

    for i in range(1, devices):
        pl.semaphore_signal(
            barrier, inc=1, device_id=device(i), device_id_type=pl.DeviceIdType.MESH
        )

    small = [
        pltpu.make_async_copy(source, target, own.at[k])
        for k, (source, target) in enumerate(
            ((owner_hbm, owner_ref), (forces_hbm, forces_ref), (slot_hbm, slot_ref), (visc_hbm, visc_ref))
        )
    ]
    for copy in small:
        copy.start()

    def weight_copy(c):
        at = pl.ds(pl.multiple_of(c * width, width), width)
        return pltpu.make_async_copy(weights_hbm.at[:, :, at], weights_ref.at[c], wsem.at[c])

    loop(0, chunks, lambda c: weight_copy(c).start())
    velocity_copy = pltpu.make_async_copy(velocity_hbm, velocity_ref, own.at[4])
    for copy in small:
        copy.wait()

    owner = owner_ref[...]
    matches = (iota((devices, blocks), 0) == owner).astype(BF16)
    earlier = (iota((blocks, blocks), 0) < iota((blocks, blocks), 1)).astype(BF16)
    counts = jnp.dot(matches, earlier, preferred_element_type=F32)
    rank = jnp.sum(counts * matches.astype(F32), axis=0, keepdims=True).astype(jnp.int32)
    target = owner * capacity + rank
    select = (iota((rows, blocks), 0) == target).astype(BF16)
    choose = (iota((markers, wide), 1) % markers == iota((markers, wide), 0)).astype(BF16)
    tiled = tn_dot(forces_ref[...], choose)
    offset = iota((blocks, wide), 1) - iota((blocks, wide), 0) * markers
    spread = jnp.where((offset >= 0) & (offset < markers), tiled, 0.0).astype(BF16)
    spread_ref[...] = jnp.dot(select, spread, preferred_element_type=F32).astype(BF16)

    number = slot_ref[...] + 1
    high = number // BASE
    ranked = iota((LANES, blocks), 0) == rank
    digits = [jnp.where(ranked, d, 0).astype(F32).astype(BF16) for d in (high, number - high * BASE)]
    meta = nt_dot(matches, digits[0]) * BASE + nt_dot(matches, digits[1])
    lane = iota((1, LANES), 1)
    viscous = jnp.zeros((1, LANES), F32)
    for x in range(cells_x):
        viscous = jnp.where(lane == VISC_LANE + x, visc_ref[x], viscous)
    meta = meta + viscous
    for d in range(devices):
        meta_ref[d] = meta[d : d + 1]

    def remote(source, target, send, receive, peer):
        return pltpu.make_async_remote_copy(
            src_ref=source,
            dst_ref=target,
            send_sem=send,
            recv_sem=receive,
            device_id=peer,
            device_id_type=pl.DeviceIdType.MESH,
        )

    def several(source, target, send, receive, number):
        at = pl.ds(0, number)
        return remote(source.at[at], target.at[at], send, receive, device(1))

    span = max(1, devices // 4)

    def tile_copy(c, i):
        return remote(
            outgoing_ref.at[index(i), c], tiles_ref.at[me, c],
            tile_send.at[0], tile_recv.at[i // span], device(i),
        )

    def tiles_come(group):
        number = span if group else span - 1
        several(outgoing_ref, tiles_ref, tile_send.at[0], tile_recv.at[group], number).wait_recv()

    def meta_copy(i):
        return remote(
            meta_ref.at[index(i)], metas_ref.at[me], meta_sem.at[0], meta_sem.at[1], device(i)
        )

    for c in range(chunks):
        weight_copy(c).wait()
        out = jnp.dot(
            spread_ref[...], weights_ref[c].reshape(wide, width), preferred_element_type=F32
        )
        if capacity % 8 == 0:
            outgoing_ref[:, c] = out.reshape(devices, capacity, width).astype(BF16)
        else:
            for d in range(devices):
                outgoing_ref[d, c] = out[d * capacity : (d + 1) * capacity].astype(BF16)
        if c == 0:
            pl.semaphore_wait(barrier, devices - 1)
        for i in range(1, devices):
            tile_copy(c, i).start()
        if c == 0:
            for i in range(1, devices):
                meta_copy(i).start()
        tiles_ref[me, c] = outgoing_ref[me, c]
    velocity_copy.start()
    metas_ref[me] = meta_ref[me]

    visc = [jnp.full((8, LANES), visc_ref[x], F32) for x in range(cells_x)]
    inverse, ratio = factor(visc)
    for x in range(last):
        local_ref[x] = inverse[x]
        local_ref[cells_x + x] = ratio[x]
    to_last, to_first = end_weights(visc, inverse, ratio)
    for x in range(last):
        weight_ref[x] = to_last[x]
        weight_ref[cells_x + x] = to_first[x]
    left, right = spikes(inverse, ratio)
    for x in range(last):
        mix_ref[x] = visc[0] * left[x]
        mix_ref[last + x] = visc[last - 1] * right[x]

    def ends_of(side):
        value = side(0)
        high, low = value * weight_ref[0], value * weight_ref[cells_x]
        for x in range(1, last):
            value = side(x)
            high = high + value * weight_ref[x]
            low = low + value * weight_ref[cells_x + x]
        return high + side(last), low

    velocity_copy.wait()

    def velocity_ends(i):
        at = pl.ds(pl.multiple_of(i * 8, 8), 8)
        for s in range(segments):
            lanes = slice(s * LANES, (s + 1) * LANES)
            high, low = ends_of(lambda x: velocity_ref[x, at, lanes])
            ends_ref[0, at, lanes] = high
            ends_ref[1, at, lanes] = low

    loop(0, rows_y // 8, velocity_ends)

    several(meta_ref, metas_ref, meta_sem.at[0], meta_sem.at[1], devices - 1).wait()
    metas = jnp.concatenate([metas_ref[d] for d in range(devices)], axis=0)
    couple(
        [
            jnp.broadcast_to(metas[:, VISC_LANE + x : VISC_LANE + x + 1], (devices, LANES))
            for x in range(cells_x)
        ],
        count_y,
        couple_ref,
    )
    lane = iota((devices, LANES), 1)
    numbers = jnp.where(lane < capacity, metas, 0.0).astype(jnp.int32)
    high = numbers // BASE
    expand = (iota((LANES, rows), 1) % capacity == iota((LANES, rows), 0)).astype(BF16)
    number = jnp.zeros((devices, rows), F32)
    for digit, base in ((high, float(BASE)), (numbers - high * BASE, 1.0)):
        number = number + base * jnp.dot(
            digit.astype(F32).astype(BF16), expand, preferred_element_type=F32
        )
    offset = iota((devices, rows), 1) - iota((devices, rows), 0) * capacity
    number = jnp.where((offset >= 0) & (offset < capacity), number, 0.0)
    number = jnp.sum(number, axis=0, keepdims=True).astype(jnp.int32) - 1
    for s in range(segments):
        place_ref[s * rows_y : (s + 1) * rows_y] = (
            iota((rows_y, rows), 0) * segments + s == number
        ).astype(BF16)

    def tile_cells(slot, x):
        c, lane = divmod(x * LANES, width)
        return tiles_ref[slot, c, :, lane : lane + LANES].astype(F32)

    def tile_ends(slot):
        at = pl.ds(pl.multiple_of(slot * capacity, capacity), capacity)
        high, low = ends_of(lambda x: tile_cells(slot, x))
        tile_ends_ref[at, :LANES] = high
        tile_ends_ref[at, LANES:] = low

    def flatten():
        for c in range(chunks):
            at = slice(c * width, (c + 1) * width)
            if capacity % 8 == 0:
                flat_ref[:, at] = tiles_ref[:, c].astype(F32).reshape(rows, width).astype(BF16)
            else:
                parts = [tiles_ref[d, c].astype(F32) for d in range(devices)]
                flat_ref[:, at] = jnp.concatenate(parts, axis=0).astype(BF16)

    if capacity % 8 == 0:
        tile_ends(me)

        for group in range(devices // span):
            if group or span > 1:
                tiles_come(group)
            for i in range(max(1, group * span), (group + 1) * span):
                tile_ends(came(i))
    else:
        for group in range(devices // span):
            if group or span > 1:
                tiles_come(group)
        flatten()

        def flat_ends(i):
            at = pl.ds(pl.multiple_of(i * 8, 8), 8)
            high, low = ends_of(lambda x: flat_ref[at, x * LANES : (x + 1) * LANES].astype(F32))
            tile_ends_ref[at, :LANES] = high
            tile_ends_ref[at, LANES:] = low

        loop(0, rows // 8, flat_ends)

    found = tile_ends_ref[...]
    coarse = found.astype(BF16)
    fine = (found - coarse.astype(F32)).astype(BF16)
    both = jnp.concatenate([coarse, fine], axis=1)
    placed = jnp.dot(place_ref[...], both, preferred_element_type=F32)
    for s in range(segments):
        lanes = slice(s * LANES, (s + 1) * LANES)
        part = placed[s * rows_y : (s + 1) * rows_y]
        for w in (0, 1):
            ends_ref[w, :, lanes] = ends_ref[w, :, lanes] + (
                part[:, w * LANES : (w + 1) * LANES] + part[:, (w + 2) * LANES : (w + 3) * LANES]
            )

    outward = ((code_ref, sides_ref, 0), (code_scale_ref, sides_scale_ref, 2))
    homeward = ((home_ref, back_ref, 4), (home_scale_ref, back_scale_ref, 6))

    def start(groups, i):
        peer = to_x(i)
        for source, target, k in groups:
            remote(
                source.at[peer], target.at[gx], line_sem.at[k], line_sem.at[k + 1], (peer, gy)
            ).start()

    def finish(groups):
        for source, target, k in groups:
            several(source, target, line_sem.at[k], line_sem.at[k + 1], count_x - 1).wait()

    def code_rows(i):
        at = pl.ds(pl.multiple_of(i * 8, 8), 8)
        pairs = []
        for s in range(segments):
            lanes = slice(s * LANES, (s + 1) * LANES)
            pairs.append((ends_ref[0, at, lanes], ends_ref[1, at, lanes]))
        most = peak([value for pair in pairs for value in pair])
        inverse = TOP / most
        codes = [pack(high, low, inverse) for high, low in pairs]
        scale = most * (1.0 / TOP)
        return codes, scale

    if share % 8 == 0:

        def code_peer(peer):
            most = None
            for k in range(share // 8):
                at = pl.ds(pl.multiple_of(peer * share + k * 8, 8), 8)
                top = peak([ends_ref[w, at, s * LANES : (s + 1) * LANES] for s in range(segments) for w in (0, 1)])
                most = top if most is None else jnp.maximum(most, top)
            inverse = TOP / most
            code_scale_ref[peer] = most * (1.0 / TOP)
            for k in range(share // 8):
                at = pl.ds(pl.multiple_of(peer * share + k * 8, 8), 8)
                for s in range(segments):
                    lanes = slice(s * LANES, (s + 1) * LANES)
                    code_ref[peer, k * 8 : (k + 1) * 8, lanes] = pack(
                        ends_ref[0, at, lanes], ends_ref[1, at, lanes], inverse
                    )

        for i in range(1, count_x):
            code_peer(to_x(i))
            start(outward, i)
        code_peer(gx)
    else:
        group = 8 // share
        for i in range(rows_y // 8):
            codes, scale = code_rows(i)
            for k in range(group):
                code_scale_ref[i * group + k] = scale
                for s in range(segments):
                    code_ref[i * group + k, :, s * LANES : (s + 1) * LANES] = codes[s][k * share : (k + 1) * share]
        for i in range(1, count_x):
            start(outward, i)
    sides_ref[gx] = code_ref[gx]
    sides_scale_ref[gx] = code_scale_ref[gx]

    if capacity % 8 == 0:
        flatten()
    for s in range(segments):
        lanes = slice(s * LANES, (s + 1) * LANES)
        rhs_ref[...] = jnp.dot(place_ref[s * rows_y : (s + 1) * rows_y], flat_ref[:, : last * LANES], preferred_element_type=F32)

        def solve(i):
            at = pl.ds(pl.multiple_of(i * 8, 8), 8)
            values = []
            for x in range(last):
                side = velocity_ref[x, at, lanes] + rhs_ref[at, x * LANES : (x + 1) * LANES]
                side = side * local_ref[x]
                values.append(side + local_ref[cells_x + x] * values[-1] if x else side)
            value = values[-1]
            inner_ref[last - 1, at, lanes] = value
            for x in range(last - 2, -1, -1):
                value = values[x] + local_ref[cells_x + x] * value
                inner_ref[x, at, lanes] = value

        loop(0, rows_y // 8, solve, unroll=2)

    finish(outward)

    most = jnp.full((share, LANES), 0.0, F32)
    for s in range(segments):
        lanes = slice(s * LANES, (s + 1) * LANES)
        values = []
        after = None
        sides = [unpack(sides_ref[d, :, lanes], sides_scale_ref[d]) for d in range(count_x)]
        for d in range(count_x):
            side = sides[d][0]
            if d + 1 < count_x:
                side = side + couple_ref[3, d : d + 1, :] * sides[d + 1][1]
            if d:
                side = side - couple_ref[2, d : d + 1, :] * values[-1]
            values.append(side * couple_ref[0, d : d + 1, :])
        value = values[-1]
        solved_ref[count_x - 1, :, lanes] = value
        most = jnp.maximum(most, jnp.abs(value))
        for d in range(count_x - 2, -1, -1):
            value = values[d] - couple_ref[1, d : d + 1, :] * value
            solved_ref[d, :, lanes] = value
            most = jnp.maximum(most, jnp.abs(value))

    most = jnp.maximum(jnp.max(most, axis=0, keepdims=True), TINY)
    inverse = TOP / most
    scale = most * (1.0 / TOP)

    def home_code(d):
        home_scale_ref[d] = scale
        before = jnp.where(d > 0, 1.0, 0.0)
        for s in range(segments):
            lanes = slice(s * LANES, (s + 1) * LANES)
            home_ref[d, :, lanes] = pack(
                solved_ref[d, :, lanes], solved_ref[jnp.maximum(d - 1, 0), :, lanes] * before, inverse
            )

    for i in range(1, count_x):
        home_code(to_x(i))
        start(homeward, i)
    home_code(gx)
    back_ref[gx] = home_ref[gx]
    back_scale_ref[gx] = home_scale_ref[gx]
    several(outgoing_ref, tiles_ref, tile_send.at[0], tile_recv.at[0], devices - 1).wait_send()
    finish(homeward)


def step(viscosity, forces, weights, owner, slots, velocity, grid_x, grid_y, capacity):
    cells_x, cells_y, cells_z = velocity.shape
    blocks, markers, cells = weights.shape
    devices = grid_x * grid_y
    rows = devices * capacity
    share = cells_y // grid_x
    chunks = 4
    dma = pltpu.SemaphoreType.DMA
    vmem = pltpu.VMEM
    anywhere = pl.BlockSpec(memory_space=pl.ANY)
    whole = pl.BlockSpec(memory_space=pltpu.VMEM)
    line = (grid_x, share, cells_z)
    line_scale = (grid_x, 1, LANES)

    def keep(value):
        return pltpu.with_memory_space_constraint(value, pltpu.HBM)

    return pl.pallas_call(
        functools.partial(step_kernel, grid_x, grid_y, capacity, chunks),
        out_shape=(
            jax.ShapeDtypeStruct((cells_x - 1, cells_y, cells_z), F32),
            jax.ShapeDtypeStruct(line, jnp.int32),
            jax.ShapeDtypeStruct(line_scale, F32),
            jax.ShapeDtypeStruct((2 * (cells_x - 1), 8, LANES), F32),
        ),
        in_specs=[anywhere] * 6,
        out_specs=(whole,) * 4,
        scratch_shapes=[
            pltpu.SMEM((cells_x,), F32),
            vmem((markers, blocks), BF16),
            vmem((1, blocks), jnp.int32),
            vmem((1, blocks), jnp.int32),
            vmem((chunks, blocks, markers, cells // chunks), BF16),
            vmem((cells_x, cells_y, cells_z), F32),
            vmem((rows, blocks * markers), BF16),
            vmem((devices, chunks, capacity, cells // chunks), BF16),
            vmem((devices, chunks, capacity, cells // chunks), BF16),
            vmem((devices, 1, LANES), F32),
            vmem((devices, 1, LANES), F32),
            vmem((cells_z // LANES * cells_y, rows), BF16),
            vmem((rows, 2 * LANES), F32),
            vmem((2, cells_y, cells_z), F32),
            vmem((2 * cells_x, 8, LANES), F32),
            vmem((2 * cells_x, 8, LANES), F32),
            vmem((4, grid_x, LANES), F32),
            vmem(line, jnp.int32),
            vmem(line_scale, F32),
            vmem(line, jnp.int32),
            vmem(line_scale, F32),
            vmem(line, F32),
            vmem(line, jnp.int32),
            vmem(line_scale, F32),
            vmem((cells_y, (cells_x - 1) * LANES), F32),
            vmem((rows, cells), BF16),
            dma((5,)),
            dma((chunks,)),
            dma((1,)),
            dma((4,)),
            dma((2,)),
            dma((8,)),
        ],
        compiler_params=pltpu.CompilerParams(
            collective_id=0, has_side_effects=True, vmem_limit_bytes=40 << 20
        ),
    )(
        keep(viscosity), keep(forces), keep(weights), keep(owner), keep(slots), keep(velocity)
    )


def rows_of(ref, i):
    rows = ref.shape[1]
    if rows % 8 == 0:
        start = pl.multiple_of(lax.rem(i * 8, rows), 8)
        return lambda lane: ref[i * 8 // rows, pl.ds(start, 8), lane]
    share = 8 // rows
    return lambda lane: jnp.concatenate([ref[i * share + k, :, lane] for k in range(share)], axis=0)


def scale_of(ref, i, rows):
    if rows % 8 == 0:
        return ref[i * 8 // rows]
    share = 8 // rows
    parts = [jnp.broadcast_to(ref[i * share + k], (rows, LANES)) for k in range(share)]
    return jnp.concatenate(parts, axis=0)


def final_kernel(parts, inner_ref, back_ref, scale_ref, mix_ref, out_hbm, out_ref, sem):
    count, rows_y, cells_z = inner_ref.shape
    rows = rows_y // parts

    def copy(p):
        at = pl.ds(pl.multiple_of(p * rows, 8), rows)
        return pltpu.make_async_copy(out_ref.at[:, at, :], out_hbm.at[:, at, :], sem.at[p])

    def chunk(i):
        at = pl.ds(pl.multiple_of(i * 8, 8), 8)
        codes = rows_of(back_ref, i)
        scale = scale_of(scale_ref, i, back_ref.shape[1])
        for c in range(cells_z // LANES):
            lane = slice(c * LANES, (c + 1) * LANES)
            last, before = unpack(codes(lane), scale)
            for x in range(count):
                out_ref[x, at, lane] = (
                    inner_ref[x, at, lane] + mix_ref[x] * before + mix_ref[count + x] * last
                )
            out_ref[count, at, lane] = last

    def part(p, carry):
        for k in range(rows // 8):
            chunk(p * (rows // 8) + k)
        copy(p).start()
        return carry

    def done(p, carry):
        copy(p).wait()
        return carry

    lax.fori_loop(0, parts, part, 0)
    lax.fori_loop(0, parts, done, 0)


def final(inner, back, scale, mix):
    count, cells_y, cells_z = inner.shape
    parts = 8
    shape = (count + 1, cells_y, cells_z)
    return pl.pallas_call(
        functools.partial(final_kernel, parts),
        out_shape=jax.ShapeDtypeStruct(shape, F32),
        in_specs=[pl.BlockSpec(memory_space=pltpu.VMEM)] * 4,
        out_specs=pl.BlockSpec(memory_space=pl.ANY),
        scratch_shapes=[pltpu.VMEM(shape, F32), pltpu.SemaphoreType.DMA((parts,))],
        compiler_params=pltpu.CompilerParams(vmem_limit_bytes=24 << 20),
    )(inner, back, scale, mix)


def per_device(velocity, viscosity, marker_forces, spread_weights, block_owner, tile_slot):
    grid_x, grid_y = lax.axis_size("gx"), lax.axis_size("gy")
    blocks = spread_weights.shape[0]
    capacity = max(2, 2 * blocks // (grid_x * grid_y))
    inner, back, scale, mix = step(
        viscosity,
        marker_forces.T,
        spread_weights,
        block_owner.reshape(1, blocks),
        tile_slot.reshape(1, blocks),
        velocity,
        grid_x,
        grid_y,
        capacity,
    )
    return final(inner, back, scale, mix)


def solution(mesh):
    placed = (
        P("gx", "gy", None),
        P("gx"),
        P(("gx", "gy"), None),
        P(("gx", "gy"), None, None),
        P(("gx", "gy"), None),
        P(("gx", "gy")),
    )
    return jax.shard_map(
        per_device, mesh=mesh, in_specs=placed, out_specs=P("gx", "gy", None), check_vma=False
    )
```
